512 devices in a mesh: dp: 64 (over z, y), tensor: 8 (over x, core).
Axes of the slice: x: 4, y: 8, z: 8, core: 2. Of those that a mesh axis runs over, the one named last changes fastest.
Arguments:
- tokens: bfloat16 [8192, 2048], P('dp'), may hold values from -8 to 8
- grad_out: bfloat16 [8192, 2048], P('dp'), may hold values from -6 to 6
- route_ids: int32 [8192, 4], P('dp'), may hold values from 0 to 59, as said below
- expert_map: int32 [60], replicated, may hold values from 0 to 63, as said below
- router: bfloat16 [2048, 60], replicated, may hold values from -1 to 1
- shared_gate: bfloat16 [2048], replicated, may hold values from -0.125 to 0.125
- sh_gate: bfloat16 [2048, 2816], P('dp', 'tensor'), may hold values from -0.125 to 0.125
- sh_up: bfloat16 [2048, 2816], P('dp', 'tensor'), may hold values from -0.125 to 0.125
- sh_down: bfloat16 [2816, 2048], P('tensor', 'dp'), may hold values from -0.109375 to 0.109375
- ex_gate: bfloat16 [64, 2048, 1408], P('dp', None, 'tensor'), may hold values from -0.125 to 0.125
- ex_up: bfloat16 [64, 2048, 1408], P('dp', None, 'tensor'), may hold values from -0.125 to 0.125
- ex_down: bfloat16 [64, 1408, 2048], P('dp', 'tensor'), may hold values from -0.15625 to 0.15625
Outputs:
- mixed: bfloat16 [8192, 2048], P('dp', 'tensor')
- grad_tokens: bfloat16 [8192, 2048], P('dp', 'tensor')
The draws below stay inside these ranges and needn't reach their ends.
Inputs may be any that keep to these rules, and one draw needn't show every extreme that they name: `route_ids`: each row names 4 different experts. Within the rows of one device (aligned blocks of 128 rows), no expert is named more than 9 times over all 4 columns, and some expert is named exactly 9 times. Entries are distinct. Expert e uses the weights of slot expert_map[e]; slot s is held by index s // 1 of dp. Slots that no expert names are not used.
All inputs are finite; a program needn't handle non-finite values.
Results may differ from the reference program's by a relative error of at most 0.011.
Values may be sent and summed in bfloat16 or wider, within the bound.
A program may use at most 64 MiB of HBM per device.

```python
import math
import jax
import jax.numpy as jnp
from jax import lax

D = 2048
F = 1408
EXPERTS = 60
TOP = 4
SH = 2816
TOK_DEV = 128
TOKENS = 8192
SLOTS = 64
CAP = 9
N_DP = 64
N_TENSOR = 8


def draw_expert_map(key, part):
    slot_order = jax.random.permutation(jax.random.fold_in(key, 11), SLOTS)
    return slot_order[:EXPERTS].astype(jnp.int32)


def route_block(block_key):
    key_order, key_keep, key_rows, key_roll = jax.random.split(block_key, 4)
    expert_order = jax.random.permutation(key_order, EXPERTS).astype(jnp.int32)
    instance_count = EXPERTS * CAP
    row_count = TOK_DEV * TOP
    remaining = CAP + jax.random.permutation(key_keep, instance_count - CAP).astype(jnp.int32)
    keep_order = jnp.concatenate([jnp.arange(CAP, dtype=jnp.int32), remaining])
    kept_mask = jnp.zeros((instance_count,), jnp.int32).at[keep_order[:row_count]].set(1)
    kept_index = jnp.nonzero(kept_mask, size=row_count)[0].astype(jnp.int32)
    expert_named = expert_order[kept_index // CAP]
    route_grid = expert_named.reshape(TOP, TOK_DEV).T
    row_order = jax.random.permutation(key_rows, TOK_DEV).astype(jnp.int32)
    route_grid = route_grid[row_order]
    roll_by = jax.random.randint(key_roll, (TOK_DEV, 1), 0, TOP, dtype=jnp.int32)
    column_order = (jnp.arange(TOP, dtype=jnp.int32)[None, :] + roll_by) % TOP
    return jnp.take_along_axis(route_grid, column_order, axis=1).astype(jnp.int32)


def route_table(key):
    block_keys = jax.random.split(jax.random.fold_in(key, 21), TOKENS // TOK_DEV)
    return jax.vmap(route_block)(block_keys).reshape(TOKENS, TOP).astype(jnp.int32)


def expert_directions(key):
    return jnp.clip(jax.random.normal(jax.random.fold_in(key, 31), (EXPERTS, D), jnp.float32), -5.0, 5.0)


def draw_route_ids(key, part):
    return route_table(key)


def draw_tokens(key, part):
    routes = route_table(key)
    onehot = jnp.sum((routes[:, :, None] == jnp.arange(EXPERTS, dtype=jnp.int32)[None, None, :]).astype(jnp.float32), axis=1)
    lifted = jnp.dot(onehot, expert_directions(key), precision=lax.Precision.HIGHEST)
    base_noise = jnp.clip(jax.random.normal(jax.random.fold_in(key, 41), (TOKENS, D), jnp.float32), -6.0, 6.0)
    values = base_noise + 6.5 / math.sqrt(D) * lifted
    return jnp.clip(values, -8.0, 8.0).astype(jnp.bfloat16)


def draw_router(key, part):
    directions = expert_directions(key)
    spread = jnp.clip(jax.random.normal(jax.random.fold_in(key, 51), (EXPERTS, D), jnp.float32), -5.0, 5.0)
    return (jnp.transpose(directions + spread) * (0.75 / math.sqrt(D))).astype(jnp.bfloat16)


def shard_levels(own_key, extent, cuts, smallest, top_value):
    gain = 1.0
    for dim, shards_of in cuts:
        draws = jax.random.uniform(jax.random.fold_in(jax.random.fold_in(own_key, 6), dim), (shards_of,), jnp.float32, smallest / len(cuts), top_value / len(cuts))
        gain = gain * jnp.repeat(jnp.exp(draws), extent[dim] // shards_of).reshape((-1,) + (1,) * (len(extent) - 1 - dim))
    return gain


def gaussian(key, shape, scale, limit, cuts=(), kind=jnp.bfloat16):
    drawn = scale * jax.random.normal(key, shape, jnp.float32)
    if cuts:
        drawn = drawn * shard_levels(key, shape, cuts, -0.22, 0.18)
    return jnp.clip(drawn, -limit, limit).astype(kind)


def setup_inputs(seed: int = 0) -> dict:
    keys = jax.random.split(jax.random.key(seed), 13)
    tokens = draw_tokens(jax.random.fold_in(keys[12], 71), 0)
    grad_out = gaussian(keys[1], (TOKENS, D), 1.0, 6.0, ((0, 64),))
    route_ids = draw_route_ids(jax.random.fold_in(keys[12], 71), 0)
    expert_map = draw_expert_map(jax.random.fold_in(keys[12], 71), 0)
    router = draw_router(jax.random.fold_in(keys[12], 71), 0)
    shared_gate = gaussian(keys[5], (D,), D ** -0.5, 0.125)
    sh_gate = gaussian(keys[6], (D, SH), D ** -0.5, 0.125, ((0, 64), (1, 8)))
    sh_up = gaussian(keys[7], (D, SH), D ** -0.5, 0.125, ((0, 64), (1, 8)))
    sh_down = gaussian(keys[8], (SH, D), SH ** -0.5, 0.109375, ((0, 8), (1, 64)))
    ex_gate = gaussian(keys[9], (SLOTS, D, F), D ** -0.5, 0.125, ((0, 64), (2, 8)))
    ex_up = gaussian(keys[10], (SLOTS, D, F), D ** -0.5, 0.125, ((0, 64), (2, 8)))
    ex_down = gaussian(keys[11], (SLOTS, F, D), F ** -0.5, 0.15625, ((0, 64), (1, 8)))
    return dict(tokens=tokens, grad_out=grad_out, route_ids=route_ids, expert_map=expert_map, router=router, shared_gate=shared_gate, sh_gate=sh_gate, sh_up=sh_up, sh_down=sh_down, ex_gate=ex_gate, ex_up=ex_up, ex_down=ex_down)


def silu_pair(pre_gate):
    sigmoid_val = 1.0 / (1.0 + jnp.exp(-pre_gate))
    return pre_gate * sigmoid_val, sigmoid_val * (1.0 + pre_gate * (1.0 - sigmoid_val))


def contract_last(left, right):
    return lax.dot_general(left, right, (((1,), (1,)), ((), ())), preferred_element_type=jnp.float32)


def expert_block(rows_in, rows_cot, w_gate, w_up, w_down):
    pre_gate = jnp.dot(rows_in, w_gate, preferred_element_type=jnp.float32)
    pre_up = jnp.dot(rows_in, w_up, preferred_element_type=jnp.float32)
    active, derivative = silu_pair(pre_gate)
    hidden = (active * pre_up).astype(jnp.bfloat16)
    result = jnp.dot(hidden, w_down, preferred_element_type=jnp.float32)
    grad_hidden = contract_last(rows_cot, w_down)
    grad_gate = (grad_hidden * pre_up * derivative).astype(jnp.bfloat16)
    grad_up = (grad_hidden * active).astype(jnp.bfloat16)
    backward = contract_last(grad_gate, w_gate) + contract_last(grad_up, w_up)
    return result, backward


def contract_last_highest(left, right):
    return lax.dot_general(left, right, (((1,), (1,)), ((), ())), precision=lax.Precision.HIGHEST, preferred_element_type=jnp.float32)


def reference(tokens, grad_out, route_ids, expert_map, router, shared_gate, sh_gate, sh_up, sh_down, ex_gate, ex_up, ex_down):
    rows_dev = TOK_DEV * TOP
    width_part = F // N_TENSOR
    group_ids = route_ids.reshape(N_DP, rows_dev)
    chosen = (group_ids[:, :, None] == jnp.arange(EXPERTS, dtype=jnp.int32)[None, None, :]).astype(jnp.int32)
    earlier = jnp.sum((jnp.cumsum(chosen, axis=1) - chosen) * chosen, axis=2).astype(jnp.int32)
    slot_of = expert_map[group_ids].astype(jnp.int32)
    position = jnp.arange(N_DP, dtype=jnp.int32)[:, None] * CAP + earlier
    token_of = jnp.arange(N_DP * rows_dev, dtype=jnp.int32).reshape(N_DP, rows_dev) // TOP
    source = jnp.full((SLOTS, N_DP * CAP), TOKENS, jnp.int32).at[slot_of, position].set(token_of)
    zero_row = jnp.zeros((1, D), jnp.bfloat16)
    padded_in = jnp.concatenate([tokens, zero_row], axis=0)
    padded_cot = jnp.concatenate([grad_out, zero_row], axis=0)

    def run_slot(operands):
        src_rows, w_gate, w_up, w_down = operands
        rows_in = jnp.take(padded_in, src_rows, axis=0)
        rows_cot = jnp.take(padded_cot, src_rows, axis=0)
        total_out = jnp.zeros((N_DP * CAP, D), jnp.float32)
        total_back = jnp.zeros((N_DP * CAP, D), jnp.float32)
        for block_idx in range(N_TENSOR):
            low_col = block_idx * width_part
            high_col = low_col + width_part
            result, backward = expert_block(rows_in, rows_cot, w_gate[:, low_col:high_col], w_up[:, low_col:high_col], w_down[low_col:high_col, :])
            total_out = total_out + lax.optimization_barrier(result.astype(jnp.bfloat16)).astype(jnp.float32)
            total_back = total_back + lax.optimization_barrier(backward.astype(jnp.bfloat16)).astype(jnp.float32)
        return total_out, total_back

    slot_out, slot_back = lax.map(run_slot, (source, ex_gate, ex_up, ex_down))
    flat_slot = slot_of.reshape(-1)
    flat_pos = position.reshape(-1)
    expert_out = slot_out[flat_slot, flat_pos].reshape(TOKENS, TOP, D)
    expert_back = slot_back[flat_slot, flat_pos].reshape(TOKENS, TOP, D)

    logits = jnp.dot(tokens, router, preferred_element_type=jnp.float32)
    exp_logit = jnp.exp(logits)
    prob_table = exp_logit / jnp.sum(exp_logit, axis=1, keepdims=True)
    picked = (route_ids[:, :, None] == jnp.arange(EXPERTS, dtype=jnp.int32)[None, None, :]).astype(jnp.float32)
    gate_weights = jnp.sum(picked * prob_table[:, None, :], axis=2)

    sh_out, sh_back = expert_block(tokens, grad_out, sh_gate, sh_up, sh_down)
    shared_scale = 1.0 / (1.0 + jnp.exp(-jnp.dot(tokens, shared_gate, preferred_element_type=jnp.float32)))

    mixed = jnp.sum(gate_weights[:, :, None] * expert_out, axis=1) + shared_scale[:, None] * sh_out
    cot_full = grad_out.astype(jnp.float32)
    out_dots = jnp.sum(cot_full[:, None, :] * expert_out, axis=2)
    shared_dots = jnp.sum(cot_full * sh_out, axis=1)
    grad_prob = jnp.sum(picked * out_dots[:, :, None], axis=1)
    dlogits = prob_table * (grad_prob - jnp.sum(gate_weights * out_dots, axis=1, keepdims=True))
    grad_router = contract_last_highest(dlogits, router.astype(jnp.float32))
    slope_term = shared_dots * shared_scale * (1.0 - shared_scale)
    grad_total = jnp.sum(gate_weights[:, :, None] * expert_back, axis=1) + shared_scale[:, None] * sh_back
    grad_total = grad_total + grad_router + slope_term[:, None] * shared_gate.astype(jnp.float32)[None, :]
    return mixed.astype(jnp.bfloat16), grad_total.astype(jnp.bfloat16)
```

```python
import jax
import jax.numpy as jnp
from jax import lax
from jax.experimental import pallas as pl
from jax.experimental.pallas import tpu as pltpu
from jax.sharding import PartitionSpec as P

MESH = pl.DeviceIdType.MESH
F32 = jnp.float32
BF16 = jnp.bfloat16
RING = 8
XS = 4
CAP = 9
HALF = 32
TOK = 128
WIDTH = 2048
QUARTER = WIDTH // XS
EIGHTH = QUARTER // 2
PACK = 2 * QUARTER + 128
HID = 176
SHID = 352
SPAD = 384
MAIN = HALF * 8
ROWS = HALF * CAP


def mm(a, b):
    return jnp.dot(a, b, preferred_element_type=F32)


def nt(a, b):
    return lax.dot_general(a, b, (((1,), (1,)), ((), ())), preferred_element_type=F32)


def halves(v):
    high = v.astype(BF16)
    return high, (v - high.astype(F32)).astype(BF16)


def silu_pair(v):
    s = 1.0 / (1.0 + jnp.exp(-v))
    return v * s, s * (1.0 + v * (1.0 - s))


def iota(shape, dim):
    return lax.broadcasted_iota(jnp.int32, shape, dim)


def one_hot(mask):
    return jnp.where(mask, 1.0, 0.0).astype(BF16)


def unpack_into(rows_ref, blocks):
    flat = blocks.astype(F32).reshape(MAIN, PACK)
    rows_ref[0:MAIN, :] = flat[:, : 2 * QUARTER].astype(BF16)
    extra = flat[:, 2 * QUARTER :].astype(BF16)
    row, col = iota((HALF, MAIN), 0), iota((HALF, MAIN), 1)
    for q in range(8):
        ninth = mm(one_hot(col == row * 8 + q), extra)
        rows_ref[MAIN:ROWS, q * 128 : (q + 1) * 128] = ninth.astype(BF16)


def pack(main, ninth):
    sub = iota((MAIN, 128), 0) % 8
    extra = jnp.zeros((MAIN, 128), F32)
    for q in range(8):
        extra = jnp.where(sub == q, ninth[:, q * 128 : (q + 1) * 128], extra)
    return main.reshape(HALF, 8, 2 * QUARTER), extra.reshape(HALF, 8, 128)


def body(
    tok, cot, ids, emap, router, sgate, sh_own, wg_in, wu_in, wd_in,
    mixed_o, grad_o,
    send, gat, wg, wu, wd, xrow, acc, hid, gg, gu, outs, rs_a, rs_b, rs_l, rs_r,
    ret_s, ret_r, shw, sh_s, sh_r, px_s, px_r, dx_s, dx_r, sh_acc,
    local_sem, w_send, w_recv, d_send, d_recv, x_send, x_recv, rs_send, rs_recv,
    t_send, t_recv, p1_send, p1_recv, ra_send, ra_recv, la_send, la_recv,
    s_send, s_recv, px_sem, dx_send, dx_recv,
):
    dp = lax.axis_index("dp")
    tp = lax.axis_index("tensor")
    x, c = tp // 2, tp % 2
    mine = dp // 2
    parity = dp % 2
    peer_t = x * 2 + parity
    to_self = parity == c
    right = ((x + 1) % XS) * 2 + c
    left = ((x + XS - 1) % XS) * 2 + c
    opposite = ((x + 2) % XS) * 2 + c
    x1, x2, x3 = (x + 1) % XS, (x + 2) % XS, (x + 3) % XS
    zc, yc = dp // RING, dp % RING
    a_me = jnp.where(c == 0, yc, zc)
    b_me = jnp.where(c == 0, zc, yc)

    def line(a, b):
        return a * (1 + 7 * c) + b * (8 - 7 * c)

    def remote(src, dst, ssem, rsem, d, t):
        return pltpu.make_async_remote_copy(
            src_ref=src, dst_ref=dst, send_sem=ssem, recv_sem=rsem, device_id=(d, t), device_id_type=MESH
        )

    def drain(ref, sem):
        pltpu.make_async_copy(ref, ref, sem).wait()

    barrier = pltpu.get_barrier_semaphore()

    def greet(d, t):
        pl.semaphore_signal(barrier, inc=1, device_id=(d, t), device_id_type=MESH)

    def greet_peer(i, carry):
        d = 2 * i + c

        @pl.when(jnp.logical_not(jnp.logical_and(d == dp, to_self)))
        def _():
            greet(d, peer_t)

        return carry

    lax.fori_loop(0, HALF, greet_peer, 0)
    for off in range(1, 8):
        greet(dp, (tp + off) % 8)
        greet(line((a_me + off) % RING, b_me), tp)
    b_right = line(a_me, (b_me + 1) % RING)
    b_left = line(a_me, (b_me + 7) % RING)
    greet(b_right, tp)
    greet(b_left, tp)

    loads = [
        pltpu.make_async_copy(wg_in, wg.at[0], local_sem.at[0]),
        pltpu.make_async_copy(wu_in, wu.at[0], local_sem.at[1]),
        pltpu.make_async_copy(wd_in, wd.at[0], local_sem.at[2]),
        pltpu.make_async_copy(sh_own, shw.at[dp], local_sem.at[3]),
    ]
    for copy in loads:
        copy.start()

    place = iota((64, 64), 0)
    slot = 2 * (place % HALF) + place // HALF
    slot_map = jnp.where(slot == emap[...], 1.0, 0.0)
    slot_expert = slot_map.astype(BF16)
    expert = iota((64, TOK), 0)
    named = jnp.zeros((64, TOK), F32)
    for k in range(4):
        named = named + jnp.where(expert == ids[k : k + 1, :], 1.0, 0.0)
    chosen = mm(slot_expert, named.astype(BF16))
    before = one_hot(iota((TOK, TOK), 0) < iota((TOK, TOK), 1))
    rank1 = chosen * (mm(chosen.astype(BF16), before) + 1.0)
    rank1_b = rank1.astype(BF16)
    spread = one_hot(iota((MAIN, 64), 1) == c * HALF + iota((MAIN, 64), 0) // 8)
    wide = mm(spread, rank1_b)
    pick_main = one_hot(wide == (iota((MAIN, TOK), 0) % 8 + 1).astype(F32))
    pick_nine = one_hot(wide == float(CAP))
    quarter_cols = pl.ds(pl.multiple_of(x * QUARTER, 128), QUARTER)
    table = jnp.concatenate([tok[:, quarter_cols], cot[:, quarter_cols]], axis=1)
    block, extra = pack(mm(pick_main, table), mm(pick_nine, table))
    send[:, :, : 2 * QUARTER] = block.astype(BF16)
    send[:, :, 2 * QUARTER :] = extra.astype(BF16)

    pl.semaphore_wait(barrier, HALF + 16 - to_self.astype(jnp.int32))

    def a2a(src, dst, ssem, rsem):
        def step(n, carry):
            i = (mine + n) % HALF
            d = 2 * i + c
            own = jnp.logical_and(d == dp, to_self)

            @pl.when(own)
            def _():
                pltpu.make_async_copy(src.at[i], dst(mine), rsem).start()

            @pl.when(jnp.logical_not(own))
            def _():
                remote(src.at[i], dst(mine), ssem, rsem, d, peer_t).start()

            return carry

        lax.fori_loop(0, HALF, step, 0)

    def a2a_sent(src, ssem):
        @pl.when(to_self)
        def _():
            drain(src.at[0 : HALF - 1], ssem)

        @pl.when(jnp.logical_not(to_self))
        def _():
            drain(src, ssem)

    a2a(send, lambda i: gat.at[x, i], d_send, d_recv)

    w_copies = [
        remote(wg_in, wg.at[1], w_send.at[0], w_recv.at[0], dp, x * 2 + 1 - c),
        remote(wu_in, wu.at[1], w_send.at[1], w_recv.at[1], dp, x * 2 + 1 - c),
        remote(wd_in, wd.at[1], w_send.at[2], w_recv.at[2], dp, x * 2 + 1 - c),
    ]
    for copy in w_copies:
        copy.start()
    for off in range(1, 8):
        remote(sh_own, shw.at[dp], p1_send, p1_recv, line((a_me + off) % RING, b_me), tp).start()

    router_s = mm(slot_expert, router[...]).astype(BF16)
    logits = nt(router_s, tok[...])
    live = jnp.sum(slot_map, axis=1, keepdims=True) > 0.5
    expd = jnp.where(live, jnp.exp(logits), 0.0)
    prob = expd / jnp.sum(expd, axis=0, keepdims=True)
    gate_w = chosen * prob
    scale = 1.0 / (
        1.0 + jnp.exp(-jnp.sum(tok[...].astype(F32) * sgate[...].astype(F32), axis=1, keepdims=True))
    )

    drain(gat.at[x], d_recv)
    g0, g1 = slice(0, HALF // 2), slice(HALF // 2, HALF)

    def x_copy(n, q, g, t):
        return remote(gat.at[q, g], gat.at[q, g], x_send.at[n], x_recv.at[n], dp, t)

    first = [x_copy(0, x, g0, right), x_copy(1, x, g1, left), x_copy(2, x, g1, right), x_copy(3, x, g0, left)]
    for copy in first:
        copy.start()

    loads[3].wait()
    drain(shw.at[0:7], p1_recv)

    def line_send(b, lo, hi, ssem, rsem, target):
        for a in range(lo, hi):
            place_ = line(a, b % RING)
            remote(shw.at[place_], shw.at[place_], ssem, rsem, target, tp).start()

    def ring_step(k):
        if k > 1:
            drain(shw.at[0:8], ra_recv.at[k - 2])
            drain(shw.at[0:8], la_recv.at[k - 2])
        hi, lo = (8, 0) if k < 4 else (4, 4)
        line_send(b_me + RING - (k - 1), 0, hi, ra_send.at[k - 1], ra_recv.at[k - 1], b_right)
        line_send(b_me + (k - 1), lo, 8, la_send.at[k - 1], la_recv.at[k - 1], b_left)

    ring_step(1)
    for copy in loads[:3]:
        copy.wait()
    for copy in w_copies:
        copy.wait_recv()

    def feed(q, start):
        unpack_into(xrow, gat[q])
        at = pl.ds(pl.multiple_of(q * QUARTER, 128), QUARTER)
        for h in range(2):
            parts = (
                mm(xrow[:, :QUARTER], wg[h, at, :]),
                mm(xrow[:, :QUARTER], wu[h, at, :]),
                nt(xrow[:, QUARTER:], wd[h, :, at]),
            )
            for n, part in enumerate(parts):
                if start:
                    acc[3 * h + n] = part
                else:
                    acc[3 * h + n] += part

    feed(x, True)
    x_copy(0, x3, g0, left).wait_recv()
    ahead = x_copy(4, x3, g0, right)
    ahead.start()
    x_copy(1, x1, g1, right).wait_recv()
    back = x_copy(5, x1, g1, left)
    back.start()
    ring_step(2)
    x_copy(2, x3, g1, left).wait_recv()
    feed(x3, False)
    x_copy(3, x1, g0, right).wait_recv()
    feed(x1, False)
    ring_step(3)
    x_copy(4, x2, g0, left).wait_recv()
    x_copy(5, x2, g1, right).wait_recv()
    feed(x2, False)

    for h in range(2):
        active, slope = silu_pair(acc[3 * h])
        up, grad_hidden = acc[3 * h + 1], acc[3 * h + 2]
        hid[h] = (active * up).astype(BF16)
        gg[h] = (grad_hidden * up * slope).astype(BF16)
        gu[h] = (grad_hidden * active).astype(BF16)

    repeat = one_hot(iota((MAIN, HALF), 1) == iota((MAIN, HALF), 0) // 8)

    def produce(q):
        at = pl.ds(pl.multiple_of(q * QUARTER, 128), QUARTER)
        out = mm(hid[0], wd[0, :, at]) + mm(hid[1], wd[1, :, at])
        grad = nt(gg[0], wg[0, at, :]) + nt(gg[1], wg[1, at, :])
        grad = grad + nt(gu[0], wu[0, at, :]) + nt(gu[1], wu[1, at, :])
        both = jnp.concatenate([out, grad], axis=1)
        return pack(both[:MAIN], mm(repeat, both[MAIN:].astype(BF16)))

    def put(ref, packed):
        ref[:, :, : 2 * QUARTER] = packed[0].astype(BF16)
        ref[:, :, 2 * QUARTER :] = packed[1].astype(BF16)

    put(outs.at[0], produce(x2))
    rs_copies = [
        remote(outs.at[0, g0], rs_a, rs_send.at[0], rs_recv.at[0], dp, right),
        remote(outs.at[0, g1], rs_b, rs_send.at[1], rs_recv.at[1], dp, left),
        remote(outs.at[1], rs_l, rs_send.at[2], rs_recv.at[2], dp, right),
        remote(outs.at[2], rs_r, rs_send.at[3], rs_recv.at[3], dp, left),
    ]
    rs_copies[0].start()
    rs_copies[1].start()
    put(outs.at[1], produce(x1))
    put(outs.at[2], produce(x3))
    rs_copies[0].wait_recv()
    outs[1, g0] = (outs[1, g0].astype(F32) + rs_a[...].astype(F32)).astype(BF16)
    rs_copies[2].start()
    rs_copies[1].wait_recv()
    outs[2, g1] = (outs[2, g1].astype(F32) + rs_b[...].astype(F32)).astype(BF16)
    rs_copies[3].start()

    put(ret_s, produce(x))

    ring_step(4)
    drain(shw.at[0:4], ra_recv.at[3])
    drain(shw.at[0:4], la_recv.at[3])

    def shared_in(n, carry):
        cols = pl.ds(pl.multiple_of(n * QUARTER, 128), QUARTER)
        blocks = pl.ds(n * 16, 16)
        parts = (
            mm(tok[:, cols], shw[blocks, :, 0:SHID].reshape(QUARTER, SHID)),
            mm(tok[:, cols], shw[blocks, :, SPAD : SPAD + SHID].reshape(QUARTER, SHID)),
            mm(cot[:, cols], shw[blocks, :, 2 * SPAD : 2 * SPAD + SHID].reshape(QUARTER, SHID)),
        )
        for m, part in enumerate(parts):
            sh_acc[m] = part + jnp.where(n == 0, 0.0, 1.0) * sh_acc[m]
        return carry

    for m in range(3):
        sh_acc[m] = jnp.zeros((TOK, SHID), F32)
    lax.fori_loop(0, XS, shared_in, 0)
    active, slope = silu_pair(sh_acc[0])
    sh_grad = sh_acc[2]
    sh_hid = (active * sh_acc[1]).astype(BF16)
    sh_gg = (sh_grad * sh_acc[1] * slope).astype(BF16)
    sh_gu = (sh_grad * active).astype(BF16)
    dot_high, dot_low = halves(sh_hid.astype(F32) * sh_grad)
    ones_s = jnp.ones((8, SHID), BF16)
    dx_s[HALF : HALF + 8, :] = nt(ones_s, dot_high) + nt(ones_s, dot_low)

    def shared_out(q):
        blocks = pl.ds(q * 16, 16)
        out = nt(sh_hid, shw[blocks, :, 2 * SPAD : 2 * SPAD + SHID].reshape(QUARTER, SHID))
        grad = nt(sh_gg, shw[blocks, :, 0:SHID].reshape(QUARTER, SHID))
        grad = grad + nt(sh_gu, shw[blocks, :, SPAD : SPAD + SHID].reshape(QUARTER, SHID))
        return jnp.concatenate([out * scale, grad * scale], axis=1)

    rs_copies[2].wait_recv()
    rs_copies[3].wait_recv()
    ret_s[...] = (ret_s[...].astype(F32) + rs_l[...].astype(F32) + rs_r[...].astype(F32)).astype(BF16)
    a2a(ret_s, lambda i: ret_r.at[i], t_send, t_recv)

    sh_copies = []
    for n, (q, t) in enumerate(((x2, opposite), (x1, right), (x3, left))):
        sh_s[n] = shared_out(q).astype(BF16)
        copy = remote(sh_s.at[n], sh_r.at[n], s_send.at[n], s_recv.at[n], dp, t)
        copy.start()
        sh_copies.append(copy)
    total = shared_out(x)

    rank_t = rank1.T.astype(BF16)
    w_high, w_low = halves(gate_w.T)
    wide_t = nt(rank_t, spread)
    gate_t = nt(w_high, spread) + nt(w_low, spread)
    weigh_main = jnp.where(wide_t == (iota((TOK, MAIN), 1) % 8 + 1).astype(F32), gate_t, 0.0)
    spread9 = one_hot(iota((HALF, 64), 1) == c * HALF + iota((HALF, 64), 0))
    wide9_t = nt(rank_t, spread9)
    gate9_t = nt(w_high, spread9) + nt(w_low, spread9)
    weigh_nine = jnp.where(wide9_t == float(CAP), gate9_t, 0.0)
    main_high, main_low = halves(weigh_main)
    nine_high, nine_low = halves(weigh_nine)
    pick9 = one_hot(mm(spread9, rank1_b) == float(CAP))
    cot_main = mm(pick_main, table[:, QUARTER:])
    cot_nine = mm(pick9, table[:, QUARTER:])

    for copy in sh_copies:
        copy.wait_recv()

    total = total + sh_r[0].astype(F32) + sh_r[1].astype(F32) + sh_r[2].astype(F32)

    drain(ret_r, t_recv)
    unpack_into(xrow, ret_r[...])
    ones_q = jnp.ones((8, QUARTER), BF16)
    row_slot = iota((HALF, MAIN), 1) // 8 == iota((HALF, MAIN), 0)
    p_high, p_low = halves(cot_main * xrow[0:MAIN, :QUARTER].astype(F32))
    dots = nt(ones_q, p_high) + nt(ones_q, p_low)
    d_high, d_low = halves(jnp.where(row_slot, dots[0:1, :], 0.0))
    p_high, p_low = halves(cot_nine * xrow[MAIN:ROWS, :QUARTER].astype(F32))
    dots9 = nt(ones_q, p_high) + nt(ones_q, p_low)
    n_high, n_low = halves(jnp.where(iota((HALF, HALF), 0) == iota((HALF, HALF), 1), dots9[0:1, :], 0.0))
    dx_s[0:HALF, :] = mm(d_high, pick_main) + mm(d_low, pick_main) + mm(n_high, pick9) + mm(n_low, pick9)
    dx_r[tp] = dx_s[...]
    for off in range(1, 8):
        remote(dx_s, dx_r.at[tp], dx_send, dx_recv, dp, (tp + off) % 8).start()

    total = total + mm(main_high, xrow[0:MAIN, :]) + mm(main_low, xrow[0:MAIN, :])
    total = total + mm(nine_high, xrow[MAIN:ROWS, :]) + mm(nine_low, xrow[MAIN:ROWS, :])
    low = jnp.concatenate([total[:, 0:EIGHTH], total[:, QUARTER : QUARTER + EIGHTH]], axis=1)
    high = jnp.concatenate([total[:, EIGHTH:QUARTER], total[:, QUARTER + EIGHTH :]], axis=1)
    px_s[...] = jnp.where(c == 0, high, low)
    own = jnp.where(c == 0, low, high)
    px = remote(px_s, px_r, px_sem.at[0], px_sem.at[1], dp, x * 2 + 1 - c)
    px.start()

    drain(dx_r.at[0:7], dx_recv)
    even = dx_r[0] + dx_r[2] + dx_r[4] + dx_r[6]
    odd = dx_r[1] + dx_r[3] + dx_r[5] + dx_r[7]
    slot_dots = jnp.concatenate([even[0:HALF], odd[0:HALF]], axis=0)
    sh_dots = (even[HALF : HALF + 8] + odd[HALF : HALF + 8]).T[:, 0:1]
    taken = chosen * slot_dots
    dlogits = prob * (taken - jnp.sum(gate_w * slot_dots, axis=0, keepdims=True))
    l_high, l_low = halves(dlogits.T)
    router_q = mm(slot_expert, router[:, pl.ds(pl.multiple_of(tp * EIGHTH, 128), EIGHTH)]).astype(BF16)
    grad = mm(l_high, router_q) + mm(l_low, router_q)
    sg_cols = sgate[:, pl.ds(pl.multiple_of(tp * EIGHTH, 128), EIGHTH)].astype(F32)
    grad = grad + sh_dots * scale * (1.0 - scale) * sg_cols
    px.wait_recv()
    both = own + px_r[...]
    mixed_o[...] = both[:, :EIGHTH].astype(BF16)
    grad_o[...] = (both[:, EIGHTH:] + grad).astype(BF16)

    a2a_sent(send, d_send)
    a2a_sent(ret_s, t_send)
    for copy in (*w_copies, *first, ahead, back, *rs_copies, *sh_copies, px):
        copy.wait_send()
    drain(shw.at[0:7], p1_send)
    for k in range(4):
        count = 8 if k < 3 else 4
        drain(shw.at[0:count], ra_send.at[k])
        drain(shw.at[0:count], la_send.at[k])
    drain(dx_r.at[0:7], dx_send)


def shards(
    tokens, grad_out, route_ids, expert_map, router, shared_gate, sh_gate, sh_up, sh_down, ex_gate, ex_up, ex_down
):
    ids = jnp.pad(route_ids.T, ((0, 4), (0, 0)), constant_values=-1)
    emap = jnp.pad(expert_map, (0, 4), constant_values=-1).reshape(1, 64)
    router_t = jnp.pad(router.T, ((0, 4), (0, 0)))
    own = jnp.concatenate([jnp.pad(a, ((0, 0), (0, SPAD - SHID))) for a in (sh_gate, sh_up, sh_down.T)], axis=1)
    vmem = pl.BlockSpec(memory_space=pltpu.VMEM)
    hbm = pl.BlockSpec(memory_space=pl.ANY)
    dma = pltpu.SemaphoreType.DMA
    block = (HALF, 8, PACK)
    return pl.pallas_call(
        body,
        out_shape=(jax.ShapeDtypeStruct((TOK, EIGHTH), BF16), jax.ShapeDtypeStruct((TOK, EIGHTH), BF16)),
        in_specs=[vmem] * 7 + [hbm] * 3,
        out_specs=(vmem, vmem),
        scratch_shapes=[
            pltpu.VMEM(block, BF16),
            pltpu.VMEM((XS, *block), BF16),
            pltpu.VMEM((2, WIDTH, HID), BF16),
            pltpu.VMEM((2, WIDTH, HID), BF16),
            pltpu.VMEM((2, HID, WIDTH), BF16),
            pltpu.VMEM((ROWS, 2 * QUARTER), BF16),
            pltpu.VMEM((6, ROWS, HID), F32),
            pltpu.VMEM((2, ROWS, HID), BF16),
            pltpu.VMEM((2, ROWS, HID), BF16),
            pltpu.VMEM((2, ROWS, HID), BF16),
            pltpu.VMEM((3, *block), BF16),
            pltpu.VMEM((HALF // 2, 8, PACK), BF16),
            pltpu.VMEM((HALF // 2, 8, PACK), BF16),
            pltpu.VMEM(block, BF16),
            pltpu.VMEM(block, BF16),
            pltpu.VMEM(block, BF16),
            pltpu.VMEM(block, BF16),
            pltpu.VMEM((RING * RING, 32, 3 * SPAD), BF16),
            pltpu.VMEM((3, TOK, 2 * QUARTER), BF16),
            pltpu.VMEM((3, TOK, 2 * QUARTER), BF16),
            pltpu.VMEM((TOK, QUARTER), F32),
            pltpu.VMEM((TOK, QUARTER), F32),
            pltpu.VMEM((HALF + 8, TOK), F32),
            pltpu.VMEM((8, HALF + 8, TOK), F32),
            pltpu.VMEM((3, TOK, SHID), F32),
            dma((4,)), dma((3,)), dma((3,)), dma, dma, dma((6,)), dma((6,)), dma((4,)), dma((4,)),
            dma, dma, dma, dma, dma((4,)), dma((4,)), dma((4,)), dma((4,)),
            dma((3,)), dma((3,)), dma((2,)), dma, dma,
        ],
        compiler_params=pltpu.CompilerParams(
            collective_id=0, has_side_effects=True, vmem_limit_bytes=60 * 1024 * 1024
        ),
    )(
        tokens, grad_out, ids, emap, router_t, shared_gate.reshape(1, WIDTH), own,
        ex_gate.reshape(WIDTH, HID), ex_up.reshape(WIDTH, HID), ex_down.reshape(HID, WIDTH),
    )


def solution(mesh):
    placed = (
        P("dp", None), P("dp", None), P("dp", None), P(), P(), P(),
        P("dp", "tensor"), P("dp", "tensor"), P("tensor", "dp"),
        P("dp", None, "tensor"), P("dp", None, "tensor"), P("dp", "tensor", None),
    )
    return jax.shard_map(
        shards,
        mesh=mesh,
        in_specs=placed,
        out_specs=(P("dp", "tensor"), P("dp", "tensor")),
        check_vma=False,
    )
```

```python
import jax
import jax.numpy as jnp
from jax import lax
from jax.experimental import pallas as pl
from jax.experimental.pallas import tpu as pltpu
from jax.sharding import PartitionSpec as P

MESH = pl.DeviceIdType.MESH
F32 = jnp.float32
BF16 = jnp.bfloat16
RING = 8
XS = 4
CAP = 9
HALF = 32
TOK = 128
WIDTH = 2048
QUARTER = WIDTH // XS
EIGHTH = QUARTER // 2
PACK = 2 * QUARTER + 128
HID = 176
SHID = 352
SPAD = 384
MAIN = HALF * 8
ROWS = HALF * CAP


def mm(a, b):
    return jnp.dot(a, b, preferred_element_type=F32)


def nt(a, b):
    return lax.dot_general(a, b, (((1,), (1,)), ((), ())), preferred_element_type=F32)


def halves(v):
    high = v.astype(BF16)
    return high, (v - high.astype(F32)).astype(BF16)


def silu_pair(v):
    s = 1.0 / (1.0 + jnp.exp(-v))
    return v * s, s * (1.0 + v * (1.0 - s))


def iota(shape, dim):
    return lax.broadcasted_iota(jnp.int32, shape, dim)


def one_hot(mask):
    return jnp.where(mask, 1.0, 0.0).astype(BF16)


def unpack_into(rows_ref, blocks):
    flat = blocks.astype(F32).reshape(MAIN, PACK)
    rows_ref[0:MAIN, :] = flat[:, : 2 * QUARTER].astype(BF16)
    extra = flat[:, 2 * QUARTER :].astype(BF16)
    row, col = iota((HALF, MAIN), 0), iota((HALF, MAIN), 1)
    for q in range(8):
        ninth = mm(one_hot(col == row * 8 + q), extra)
        rows_ref[MAIN:ROWS, q * 128 : (q + 1) * 128] = ninth.astype(BF16)


def pack(main, ninth):
    sub = iota((MAIN, 128), 0) % 8
    extra = jnp.zeros((MAIN, 128), F32)
    for q in range(8):
        extra = jnp.where(sub == q, ninth[:, q * 128 : (q + 1) * 128], extra)
    return main.reshape(HALF, 8, 2 * QUARTER), extra.reshape(HALF, 8, 128)


def body(
    tok, cot, ids, emap, router, sgate_in, sh_gate, sh_up, sh_down, wg_in, wu_in, wd_in,
    mixed_o, grad_o,
    send, gat, wg, wu, wd, xrow, acc, hid, gg, gu, outs, rs_a, rs_b, rs_l, rs_r,
    ret_s, ret_r, shw, sh_own, sgate, sh_s, sh_r, px_s, px_r, dx_s, dx_r, sh_acc, dot_s, dot_r,
    local_sem, w_send, w_recv, d_send, d_recv, x_send, x_recv, rs_send, rs_recv,
    t_send, t_recv, p1_send, p1_recv, ra_send, ra_recv, la_send, la_recv,
    s_send, s_recv, px_sem, dx_send, dx_recv, o_send, o_recv,
):
    dp = lax.axis_index("dp")
    tp = lax.axis_index("tensor")
    x, c = tp // 2, tp % 2
    mine = dp // 2
    parity = dp % 2
    peer_t = x * 2 + parity
    to_self = parity == c
    right = ((x + 1) % XS) * 2 + c
    left = ((x + XS - 1) % XS) * 2 + c
    opposite = ((x + 2) % XS) * 2 + c
    x1, x2, x3 = (x + 1) % XS, (x + 2) % XS, (x + 3) % XS
    zc, yc = dp // RING, dp % RING
    a_me = jnp.where(c == 0, yc, zc)
    b_me = jnp.where(c == 0, zc, yc)

    def line(a, b):
        return a * (1 + 7 * c) + b * (8 - 7 * c)

    def offset(k):
        return jnp.where(k % 2 == 0, k // 2, HALF - (k + 1) // 2)

    def peer_of(k):
        return (mine + offset(k)) % HALF

    def remote(src, dst, ssem, rsem, d, t):
        return pltpu.make_async_remote_copy(
            src_ref=src, dst_ref=dst, send_sem=ssem, recv_sem=rsem, device_id=(d, t), device_id_type=MESH
        )

    def drain(ref, sem):
        pltpu.make_async_copy(ref, ref, sem).wait()

    barrier = pltpu.get_barrier_semaphore()

    def greet(d, t):
        pl.semaphore_signal(barrier, inc=1, device_id=(d, t), device_id_type=MESH)

    def greet_peer(i, carry):
        d = 2 * i + c

        @pl.when(jnp.logical_not(jnp.logical_and(d == dp, to_self)))
        def _():
            greet(d, peer_t)

        return carry

    lax.fori_loop(0, HALF, greet_peer, 0)
    for off in range(1, 8):
        greet(dp, (tp + off) % 8)
        greet(line((a_me + off) % RING, b_me), tp)
    b_right = line(a_me, (b_me + 1) % RING)
    b_left = line(a_me, (b_me + 7) % RING)
    greet(b_right, tp)
    greet(b_left, tp)

    loads = [
        pltpu.make_async_copy(wg_in, wg.at[0], local_sem.at[0]),
        pltpu.make_async_copy(wu_in, wu.at[0], local_sem.at[1]),
        pltpu.make_async_copy(wd_in, wd.at[0], local_sem.at[2]),
        pltpu.make_async_copy(sh_own, shw.at[dp], local_sem.at[3]),
    ]
    for copy in loads[:3]:
        copy.start()
    for n, piece in enumerate((sh_gate, sh_up, sh_down)):
        sh_own[:, n * SPAD : n * SPAD + SHID] = piece[...]
        sh_own[:, n * SPAD + SHID : (n + 1) * SPAD] = jnp.zeros((32, SPAD - SHID), BF16)
    for n in range(WIDTH // 128):
        sgate[:, n * 128 : (n + 1) * 128] = sgate_in[n : n + 1, :].astype(F32)

    place = iota((64, 60), 0)
    slot = 2 * (place % HALF) + place // HALF
    slot_map = jnp.where(slot == emap[...], 1.0, 0.0)
    slot_expert = slot_map.astype(BF16)
    expert = iota((60, TOK), 0)
    named = jnp.zeros((60, TOK), F32)
    for k in range(4):
        named = named + jnp.where(expert == ids[k : k + 1, :], 1.0, 0.0)
    chosen = mm(slot_expert, named.astype(BF16))
    before = one_hot(iota((TOK, TOK), 0) < iota((TOK, TOK), 1))
    rank1 = chosen * (mm(chosen.astype(BF16), before) + 1.0)
    rank1_b = rank1.astype(BF16)
    spread = one_hot(iota((MAIN, 64), 1) == c * HALF + peer_of(iota((MAIN, 64), 0) // 8))
    wide = mm(spread, rank1_b)
    pick_main = one_hot(wide == (iota((MAIN, TOK), 0) % 8 + 1).astype(F32))
    pick_nine = one_hot(wide == float(CAP))
    quarter_cols = pl.ds(pl.multiple_of(x * QUARTER, 128), QUARTER)
    table = jnp.concatenate([tok[:, quarter_cols], cot[:, quarter_cols]], axis=1)
    block, extra = pack(mm(pick_main, table), mm(pick_nine, table))
    send[:, :, : 2 * QUARTER] = block.astype(BF16)
    send[:, :, 2 * QUARTER :] = extra.astype(BF16)

    pl.semaphore_wait(barrier, HALF + 16 - to_self.astype(jnp.int32))

    def a2a(src, dst, ssem, rsem, lo, hi, sign):
        def step(k, carry):
            i = (mine + sign * offset(k) + HALF) % HALF
            own = jnp.logical_and(k == 0, to_self)

            @pl.when(own)
            def _():
                pltpu.make_async_copy(src.at[k], dst(k), rsem).start()

            @pl.when(jnp.logical_not(own))
            def _():
                remote(src.at[k], dst(k), ssem, rsem, 2 * i + c, peer_t).start()

            return carry

        lax.fori_loop(lo, hi, step, 0)

    def a2a_sent(src, ssem):
        @pl.when(to_self)
        def _():
            drain(src.at[0 : HALF - 1], ssem)

        @pl.when(jnp.logical_not(to_self))
        def _():
            drain(src, ssem)

    a2a(send, lambda k: gat.at[x, k], d_send, d_recv.at[0], 0, 16, 1)
    a2a(send, lambda k: gat.at[x, k], d_send, d_recv.at[1], 16, HALF, 1)

    loads[3].start()

    w_copies = [
        remote(wg_in, wg.at[1], w_send.at[0], w_recv.at[0], dp, x * 2 + 1 - c),
        remote(wu_in, wu.at[1], w_send.at[1], w_recv.at[1], dp, x * 2 + 1 - c),
        remote(wd_in, wd.at[1], w_send.at[2], w_recv.at[2], dp, x * 2 + 1 - c),
    ]
    for copy in w_copies:
        copy.start()
    for off in range(1, 8):
        remote(sh_own, shw.at[dp], p1_send, p1_recv, line((a_me + off) % RING, b_me), tp).start()

    router_s = mm(slot_expert, router[...]).astype(BF16)
    logits = nt(router_s, tok[...])
    live = jnp.sum(slot_map, axis=1, keepdims=True) > 0.5
    expd = jnp.where(live, jnp.exp(logits), 0.0)
    prob = expd / jnp.sum(expd, axis=0, keepdims=True)
    gate_w = chosen * prob
    scale = 1.0 / (
        1.0 + jnp.exp(-jnp.sum(tok[...].astype(F32) * sgate[...], axis=1, keepdims=True))
    )

    h = [slice(8 * n, 8 * n + 8) for n in range(4)]

    def x_copy(n, q, part, t):
        return remote(gat.at[q, part], gat.at[q, part], x_send.at[n], x_recv.at[n], dp, t)

    sent = []

    def go(copy):
        copy.start()
        sent.append(copy)

    def x_first(n, part, other):
        drain(gat.at[x, 0:16], d_recv.at[n // 6])
        go(x_copy(n, x, part, right))
        go(x_copy(n + 1, x, other, left))
        go(x_copy(n + 2, x, other, right))
        go(x_copy(n + 3, x, part, left))

    def x_forward(n, part, other):
        x_copy(n, x3, part, left).wait_recv()
        go(x_copy(n + 4, x3, part, right))
        x_copy(n + 1, x1, other, right).wait_recv()
        go(x_copy(n + 5, x1, other, left))

    x_first(0, h[0], h[1])
    x_forward(0, h[0], h[1])
    x_first(6, h[2], h[3])

    loads[3].wait()
    drain(shw.at[0:7], p1_recv)

    def line_send(b, half, ssem, rsem, target):
        for a in range(4 * half, 4 * half + 4):
            at_ = line(a, b % RING)
            remote(shw.at[at_], shw.at[at_], ssem, rsem, target, tp).start()

    def ring_step(k, half):
        n = 2 * (k - 1) + half
        if k > 1:
            drain(shw.at[0:4], ra_recv.at[n - 2])
            drain(shw.at[0:4], la_recv.at[n - 2])
        if k < 4 or half == 0:
            line_send(b_me + RING - (k - 1), half, ra_send.at[n], ra_recv.at[n], b_right)
        if k < 4 or half == 1:
            line_send(b_me + (k - 1), half, la_send.at[n], la_recv.at[n], b_left)

    ring_step(1, 0)
    ring_step(1, 1)
    for copy in loads[:3]:
        copy.wait()
    for copy in w_copies:
        copy.wait_recv()

    def feed(q, start):
        unpack_into(xrow, gat[q])
        at = pl.ds(pl.multiple_of(q * QUARTER, 128), QUARTER)
        for p in range(2):
            parts = (
                nt(xrow[:, :QUARTER], wg[p, :, at]),
                nt(xrow[:, :QUARTER], wu[p, :, at]),
                nt(xrow[:, QUARTER:], wd[p, :, at]),
            )
            for n, part in enumerate(parts):
                if start:
                    acc[3 * p + n] = part
                else:
                    acc[3 * p + n] += part

    x_copy(2, x3, h[1], left).wait_recv()
    x_copy(3, x1, h[0], right).wait_recv()
    x_copy(4, x2, h[0], left).wait_recv()
    x_copy(5, x2, h[1], right).wait_recv()
    feed(x, True)
    x_forward(6, h[2], h[3])
    ring_step(2, 0)
    ring_step(2, 1)
    x_copy(8, x3, h[3], left).wait_recv()
    feed(x3, False)
    x_copy(9, x1, h[2], right).wait_recv()
    feed(x1, False)
    x_copy(10, x2, h[2], left).wait_recv()
    x_copy(11, x2, h[3], right).wait_recv()
    feed(x2, False)

    row_dots = jnp.zeros((ROWS, 1), F32)
    for p in range(2):
        active, slope = silu_pair(acc[3 * p])
        up, grad_hidden = acc[3 * p + 1], acc[3 * p + 2]
        hid[p] = (active * up).astype(BF16)
        gg[p] = (grad_hidden * up * slope).astype(BF16)
        gu[p] = (grad_hidden * active).astype(BF16)
        row_dots = row_dots + jnp.sum(hid[p].astype(F32) * grad_hidden, axis=1, keepdims=True)

    repeat = one_hot(iota((MAIN, HALF), 1) == iota((MAIN, HALF), 0) // 8)

    def produce(q):
        at = pl.ds(pl.multiple_of(q * QUARTER, 128), QUARTER)
        out = mm(hid[0], wd[0, :, at]) + mm(hid[1], wd[1, :, at])
        grad = mm(gg[0], wg[0, :, at]) + mm(gg[1], wg[1, :, at])
        grad = grad + mm(gu[0], wu[0, :, at]) + mm(gu[1], wu[1, :, at])
        both = jnp.concatenate([out, grad], axis=1)
        return pack(both[:MAIN], mm(repeat, both[MAIN:].astype(BF16)))

    def put(ref, packed):
        ref[:, :, : 2 * QUARTER] = packed[0].astype(BF16)
        ref[:, :, 2 * QUARTER :] = packed[1].astype(BF16)

    def rs_copy(n, src, dst, t):
        return remote(src, dst, rs_send.at[n], rs_recv.at[n], dp, t)

    def add_part(ref, at, more):
        ref[at] = (ref[at].astype(F32) + more.astype(F32)).astype(BF16)

    put(outs.at[0], produce(x2))
    go(rs_copy(0, outs.at[0, h[2]], rs_a.at[0], right))
    go(rs_copy(1, outs.at[0, h[3]], rs_b.at[0], left))
    put(outs.at[1], produce(x1))
    go(rs_copy(2, outs.at[1, h[3]], rs_l.at[h[3]], right))
    put(outs.at[2], produce(x3))
    go(rs_copy(3, outs.at[2, h[2]], rs_r.at[h[2]], left))

    n_high, n_low = halves(jnp.broadcast_to(row_dots[MAIN:], (HALF, 128)))
    ninth_dots = mm(repeat, n_high) + mm(repeat, n_low)
    both_dots = jnp.where(iota((MAIN, 128), 1) < 64, jnp.broadcast_to(row_dots[:MAIN], (MAIN, 128)), ninth_dots)
    dot_s[...] = both_dots.reshape(HALF, 8, 128)

    put(ret_s, produce(x))
    a2a(dot_s, lambda k: dot_r.at[k], o_send, o_recv, 0, HALF, -1)
    ring_step(3, 0)
    rs_copy(0, outs.at[0, h[2]], rs_a.at[0], left).wait_recv()
    add_part(outs, (1, h[2]), rs_a[0])
    go(rs_copy(4, outs.at[1, h[2]], rs_l.at[h[2]], right))
    rs_copy(1, outs.at[0, h[3]], rs_b.at[0], right).wait_recv()
    add_part(outs, (2, h[3]), rs_b[0])
    go(rs_copy(5, outs.at[2, h[3]], rs_r.at[h[3]], left))
    go(rs_copy(6, outs.at[0, h[0]], rs_a.at[1], right))
    go(rs_copy(7, outs.at[0, h[1]], rs_b.at[1], left))
    go(rs_copy(8, outs.at[1, h[1]], rs_l.at[h[1]], right))
    go(rs_copy(9, outs.at[2, h[0]], rs_r.at[h[0]], left))
    ring_step(3, 1)
    ring_step(4, 0)

    far, near = slice(16, HALF), slice(0, 16)
    for n, part in ((2, h[3]), (4, h[2])):
        rs_copy(n, outs.at[1, part], rs_l.at[part], left).wait_recv()
    for n, part in ((3, h[2]), (5, h[3])):
        rs_copy(n, outs.at[2, part], rs_r.at[part], right).wait_recv()
    add_part(ret_s, far, rs_l[far].astype(F32) + rs_r[far].astype(F32))
    a2a(ret_s, lambda k: ret_r.at[k], t_send, t_recv.at[1], 16, HALF, -1)
    ring_step(4, 1)

    drain(shw.at[0:4], ra_recv.at[6])
    drain(shw.at[0:4], la_recv.at[7])

    def shared_in(n, carry):
        cols = pl.ds(pl.multiple_of(n * QUARTER, 128), QUARTER)
        blocks = pl.ds(n * 16, 16)
        parts = (
            mm(tok[:, cols], shw[blocks, :, 0:SHID].reshape(QUARTER, SHID)),
            mm(tok[:, cols], shw[blocks, :, SPAD : SPAD + SHID].reshape(QUARTER, SHID)),
            mm(cot[:, cols], shw[blocks, :, 2 * SPAD : 2 * SPAD + SHID].reshape(QUARTER, SHID)),
        )
        for m, part in enumerate(parts):
            sh_acc[m] = part + jnp.where(n == 0, 0.0, 1.0) * sh_acc[m]
        return carry

    rs_copy(6, outs.at[0, h[0]], rs_a.at[1], left).wait_recv()
    add_part(outs, (1, h[0]), rs_a[1])
    go(rs_copy(10, outs.at[1, h[0]], rs_l.at[h[0]], right))
    rs_copy(7, outs.at[0, h[1]], rs_b.at[1], right).wait_recv()
    add_part(outs, (2, h[1]), rs_b[1])
    go(rs_copy(11, outs.at[2, h[1]], rs_r.at[h[1]], left))

    for m in range(3):
        sh_acc[m] = jnp.zeros((TOK, SHID), F32)
    lax.fori_loop(0, XS, shared_in, 0)
    active, slope = silu_pair(sh_acc[0])
    sh_grad = sh_acc[2]
    sh_hid = (active * sh_acc[1]).astype(BF16)
    sh_gg = (sh_grad * sh_acc[1] * slope).astype(BF16)
    sh_gu = (sh_grad * active).astype(BF16)
    dot_high, dot_low = halves(sh_hid.astype(F32) * sh_grad)
    ones_s = jnp.ones((8, SHID), BF16)
    dx_s[HALF : HALF + 8, :] = nt(ones_s, dot_high) + nt(ones_s, dot_low)

    def shared_out(q):
        blocks = pl.ds(q * 16, 16)
        out = nt(sh_hid, shw[blocks, :, 2 * SPAD : 2 * SPAD + SHID].reshape(QUARTER, SHID))
        grad = nt(sh_gg, shw[blocks, :, 0:SHID].reshape(QUARTER, SHID))
        grad = grad + nt(sh_gu, shw[blocks, :, SPAD : SPAD + SHID].reshape(QUARTER, SHID))
        return jnp.concatenate([out * scale, grad * scale], axis=1)

    def s_copy(n, src, dst, t):
        return remote(src, dst, s_send.at[n], s_recv.at[n], dp, t)

    top, low_ = slice(0, 64), slice(64, TOK)
    sh_s[0] = shared_out(x2).astype(BF16)
    go(s_copy(0, sh_s.at[0, top], sh_r.at[0, top], right))
    go(s_copy(1, sh_s.at[0, low_], sh_r.at[0, low_], left))
    sh_s[1] = shared_out(x1).astype(BF16)
    go(s_copy(2, sh_s.at[1, low_], sh_r.at[1, low_], right))
    sh_s[2] = shared_out(x3).astype(BF16)
    go(s_copy(3, sh_s.at[2, top], sh_r.at[2, top], left))

    for n, part in ((8, h[1]), (10, h[0])):
        rs_copy(n, outs.at[1, part], rs_l.at[part], left).wait_recv()
    for n, part in ((9, h[0]), (11, h[1])):
        rs_copy(n, outs.at[2, part], rs_r.at[part], right).wait_recv()
    add_part(ret_s, near, rs_l[near].astype(F32) + rs_r[near].astype(F32))
    a2a(ret_s, lambda k: ret_r.at[k], t_send, t_recv.at[0], 0, 16, -1)

    total = shared_out(x)
    s_copy(0, sh_s.at[0, top], sh_r.at[0, top], left).wait_recv()
    add_part(sh_s, (1, top), sh_r[0, top])
    go(s_copy(4, sh_s.at[1, top], sh_r.at[1, top], right))
    s_copy(1, sh_s.at[0, low_], sh_r.at[0, low_], right).wait_recv()
    add_part(sh_s, (2, low_), sh_r[0, low_])
    go(s_copy(5, sh_s.at[2, low_], sh_r.at[2, low_], left))

    own_slot = peer_of(iota((HALF, MAIN), 1) // 8) == iota((HALF, MAIN), 0)
    gather_main = one_hot(own_slot)
    gather_nine = one_hot(jnp.logical_and(own_slot, iota((HALF, MAIN), 1) % 8 == 0))
    drain(dot_r, o_recv)
    flat_dots = dot_r[...].reshape(MAIN, 128)
    p_high, p_low = halves(pick_main.astype(F32) * flat_dots[:, 0:1])
    n_high, n_low = halves(pick_nine.astype(F32) * flat_dots[:, 64:65])
    dx_s[0:HALF, :] = mm(gather_main, p_high) + mm(gather_main, p_low) + mm(gather_nine, n_high) + mm(gather_nine, n_low)
    dx_r[tp] = dx_s[...]
    for off in range(1, 8):
        remote(dx_s, dx_r.at[tp], dx_send, dx_recv, dp, (tp + off) % 8).start()

    rank_t = rank1.T.astype(BF16)
    w_high, w_low = halves(gate_w.T)
    wide_t = nt(rank_t, spread)
    gate_t = nt(w_high, spread) + nt(w_low, spread)
    weigh_main = jnp.where(wide_t == (iota((TOK, MAIN), 1) % 8 + 1).astype(F32), gate_t, 0.0)
    spread9 = one_hot(iota((HALF, 64), 1) == c * HALF + peer_of(iota((HALF, 64), 0)))
    wide9_t = nt(rank_t, spread9)
    gate9_t = nt(w_high, spread9) + nt(w_low, spread9)
    weigh_nine = jnp.where(wide9_t == float(CAP), gate9_t, 0.0)
    main_high, main_low = halves(weigh_main)
    nine_high, nine_low = halves(weigh_nine)

    drain(dx_r.at[0:7], dx_recv)
    even = dx_r[0] + dx_r[2] + dx_r[4] + dx_r[6]
    odd = dx_r[1] + dx_r[3] + dx_r[5] + dx_r[7]
    slot_dots = jnp.concatenate([even[0:HALF], odd[0:HALF]], axis=0)
    sh_dots = (even[HALF : HALF + 8] + odd[HALF : HALF + 8]).T[:, 0:1]
    taken = chosen * slot_dots
    dlogits = prob * (taken - jnp.sum(gate_w * slot_dots, axis=0, keepdims=True))
    l_high, l_low = halves(dlogits.T)
    router_q = mm(slot_expert, router[:, pl.ds(pl.multiple_of(tp * EIGHTH, 128), EIGHTH)]).astype(BF16)
    grad = mm(l_high, router_q) + mm(l_low, router_q)
    sg_cols = sgate[:, pl.ds(pl.multiple_of(tp * EIGHTH, 128), EIGHTH)]
    grad = grad + sh_dots * scale * (1.0 - scale) * sg_cols

    s_copy(2, sh_s.at[1, low_], sh_r.at[1, low_], left).wait_recv()
    s_copy(3, sh_s.at[2, top], sh_r.at[2, top], right).wait_recv()
    s_copy(4, sh_s.at[1, top], sh_r.at[1, top], left).wait_recv()
    s_copy(5, sh_s.at[2, low_], sh_r.at[2, low_], right).wait_recv()
    total = total + sh_r[1].astype(F32) + sh_r[2].astype(F32)

    drain(ret_r.at[0:16], t_recv.at[1])
    drain(ret_r.at[0:16], t_recv.at[0])
    unpack_into(xrow, ret_r[...])
    total = total + mm(main_high, xrow[0:MAIN, :]) + mm(main_low, xrow[0:MAIN, :])
    total = total + mm(nine_high, xrow[MAIN:ROWS, :]) + mm(nine_low, xrow[MAIN:ROWS, :])
    low = jnp.concatenate([total[:, 0:EIGHTH], total[:, QUARTER : QUARTER + EIGHTH]], axis=1)
    high = jnp.concatenate([total[:, EIGHTH:QUARTER], total[:, QUARTER + EIGHTH :]], axis=1)
    px_s[...] = jnp.where(c == 0, high, low)
    own = jnp.where(c == 0, low, high)
    px = remote(px_s, px_r, px_sem.at[0], px_sem.at[1], dp, x * 2 + 1 - c)
    px.start()
    px.wait_recv()
    both = own + px_r[...]
    mixed_o[...] = both[:, :EIGHTH].astype(BF16)
    grad_o[...] = (both[:, EIGHTH:] + grad).astype(BF16)

    a2a_sent(send, d_send)
    a2a_sent(ret_s, t_send)
    a2a_sent(dot_s, o_send)
    for copy in (*w_copies, *sent, px):
        copy.wait_send()
    drain(shw.at[0:7], p1_send)
    for n in range(7):
        drain(shw.at[0:4], ra_send.at[n])
        drain(shw.at[0:4], la_send.at[n if n < 6 else 7])
    drain(dx_r.at[0:7], dx_send)


def shards(
    tokens, grad_out, route_ids, expert_map, router, shared_gate, sh_gate, sh_up, sh_down, ex_gate, ex_up, ex_down
):
    vmem = pl.BlockSpec(memory_space=pltpu.VMEM)
    hbm = pl.BlockSpec(memory_space=pl.ANY)
    dma = pltpu.SemaphoreType.DMA
    block = (HALF, 8, PACK)
    return pl.pallas_call(
        body,
        out_shape=(jax.ShapeDtypeStruct((TOK, EIGHTH), BF16), jax.ShapeDtypeStruct((TOK, EIGHTH), BF16)),
        in_specs=[vmem] * 9 + [hbm] * 3,
        out_specs=(vmem, vmem),
        scratch_shapes=[
            pltpu.VMEM(block, BF16),
            pltpu.VMEM((XS, *block), BF16),
            pltpu.VMEM((2, HID, WIDTH), BF16),
            pltpu.VMEM((2, HID, WIDTH), BF16),
            pltpu.VMEM((2, HID, WIDTH), BF16),
            pltpu.VMEM((ROWS, 2 * QUARTER), BF16),
            pltpu.VMEM((6, ROWS, HID), F32),
            pltpu.VMEM((2, ROWS, HID), BF16),
            pltpu.VMEM((2, ROWS, HID), BF16),
            pltpu.VMEM((2, ROWS, HID), BF16),
            pltpu.VMEM((3, *block), BF16),
            pltpu.VMEM((2, 8, 8, PACK), BF16),
            pltpu.VMEM((2, 8, 8, PACK), BF16),
            pltpu.VMEM(block, BF16),
            pltpu.VMEM(block, BF16),
            pltpu.VMEM(block, BF16),
            pltpu.VMEM(block, BF16),
            pltpu.VMEM((RING * RING, 32, 3 * SPAD), BF16),
            pltpu.VMEM((32, 3 * SPAD), BF16),
            pltpu.VMEM((1, WIDTH), F32),
            pltpu.VMEM((3, TOK, 2 * QUARTER), BF16),
            pltpu.VMEM((3, TOK, 2 * QUARTER), BF16),
            pltpu.VMEM((TOK, QUARTER), F32),
            pltpu.VMEM((TOK, QUARTER), F32),
            pltpu.VMEM((HALF + 8, TOK), F32),
            pltpu.VMEM((8, HALF + 8, TOK), F32),
            pltpu.VMEM((3, TOK, SHID), F32),
            pltpu.VMEM((HALF, 8, 128), F32),
            pltpu.VMEM((HALF, 8, 128), F32),
            dma((4,)), dma((3,)), dma((3,)), dma, dma((2,)), dma((12,)), dma((12,)), dma((12,)), dma((12,)),
            dma, dma((2,)), dma, dma, dma((8,)), dma((8,)), dma((8,)), dma((8,)),
            dma((6,)), dma((6,)), dma((2,)), dma, dma, dma, dma,
        ],
        compiler_params=pltpu.CompilerParams(
            collective_id=0, has_side_effects=True, vmem_limit_bytes=60 * 1024 * 1024
        ),
    )(
        tokens, grad_out, route_ids.T, expert_map.reshape(1, 60), router.T, shared_gate.reshape(16, 128),
        sh_gate, sh_up, sh_down.T,
        ex_gate.reshape(WIDTH, HID).T, ex_up.reshape(WIDTH, HID).T, ex_down.reshape(HID, WIDTH),
    )


def solution(mesh):
    placed = (
        P("dp", None), P("dp", None), P("dp", None), P(), P(), P(),
        P("dp", "tensor"), P("dp", "tensor"), P("tensor", "dp"),
        P("dp", None, "tensor"), P("dp", None, "tensor"), P("dp", "tensor", None),
    )
    return jax.shard_map(
        shards,
        mesh=mesh,
        in_specs=placed,
        out_specs=(P("dp", "tensor"), P("dp", "tensor")),
        check_vma=False,
    )
```

```python
import jax
import jax.numpy as jnp
from jax import lax
from jax.experimental import pallas as pl
from jax.experimental.pallas import tpu as pltpu
from jax.sharding import PartitionSpec as P

MESH = pl.DeviceIdType.MESH
F32 = jnp.float32
BF16 = jnp.bfloat16
RING = 8
XS = 4
CAP = 9
HALF = 32
TOK = 128
WIDTH = 2048
QUARTER = WIDTH // XS
EIGHTH = QUARTER // 2
PACK = 2 * QUARTER + 128
HID = 176
SHID = 352
SPAD = 384
MAIN = HALF * 8
OWN = 16
SETS = 4
ROWS = HALF * CAP


def mm(a, b):
    return jnp.dot(a, b, preferred_element_type=F32)


def nt(a, b):
    return lax.dot_general(a, b, (((1,), (1,)), ((), ())), preferred_element_type=F32)


def halves(v):
    high = v.astype(BF16)
    return high, (v - high.astype(F32)).astype(BF16)


def silu_pair(v):
    s = 1.0 / (1.0 + jnp.exp(-v))
    return v * s, s * (1.0 + v * (1.0 - s))


def iota(shape, dim):
    return lax.broadcasted_iota(jnp.int32, shape, dim)


def one_hot(mask):
    return jnp.where(mask, 1.0, 0.0).astype(BF16)


def unpack_into(rows_ref, blocks):
    flat = blocks.astype(F32).reshape(MAIN, PACK)
    rows_ref[0:MAIN, :] = flat[:, : 2 * QUARTER].astype(BF16)
    extra = flat[:, 2 * QUARTER :].astype(BF16)
    row, col = iota((HALF, MAIN), 0), iota((HALF, MAIN), 1)
    for q in range(8):
        ninth = mm(one_hot(col == row * 8 + q), extra)
        rows_ref[MAIN:ROWS, q * 128 : (q + 1) * 128] = ninth.astype(BF16)


def pack(main, ninth):
    sub = iota((MAIN, 128), 0) % 8
    extra = jnp.zeros((MAIN, 128), F32)
    for q in range(8):
        extra = jnp.where(sub == q, ninth[:, q * 128 : (q + 1) * 128], extra)
    return main.reshape(HALF, 8, 2 * QUARTER), extra.reshape(HALF, 8, 128)


def body(
    tok, cot, ids, emap, router, sgate_in, sh_gate, sh_up, sh_down, wg_in, wu_in, wd_in,
    result,
    send, gat, wg, wu, wd, xrow, acc, hid, gg, gu, outs, rs_a, rs_b, rs_l, rs_r,
    ret_s, ret_r, shw, sh_own, sgate, sh_s, sh_r, px_s, px_r, dx_s, dx_r, sh_acc, dot_s, dot_r, sx_s, sx_r,
    local_sem, w_send, w_recv, d_send, d_recv, x_send, x_recv, rs_send, rs_recv,
    t_send, t_recv, pr_send, pr_recv, pl_send, pl_recv, ra_send, ra_recv, la_send, la_recv,
    s_send, s_recv, px_sem, dx_send, dx_recv, o_send, o_recv, sx_send, sx_recv,
):
    dp = lax.axis_index("dp")
    tp = lax.axis_index("tensor")
    x, c = tp // 2, tp % 2
    mine = dp // 2
    parity = dp % 2
    peer_t = x * 2 + parity
    to_self = parity == c
    right = ((x + 1) % XS) * 2 + c
    left = ((x + XS - 1) % XS) * 2 + c
    opposite = ((x + 2) % XS) * 2 + c
    x1, x2, x3 = (x + 1) % XS, (x + 2) % XS, (x + 3) % XS
    zc, yc = dp // RING, dp % RING
    a_me = jnp.where(c == 0, yc, zc)
    b_me = jnp.where(c == 0, zc, yc)

    def line(a, b):
        return a * (1 + 7 * c) + b * (8 - 7 * c)

    def peer_of(k, sign=1):
        j = k // 4
        dz = jnp.where(j < 2, 1 + 4 * j, jnp.where(j < 4, 15 - 4 * j, jnp.where(j < 6, 4 * j - 16, 4 * j - 22)))
        return ((zc + sign * dz + RING) % RING) * 4 + (yc // 2 + sign * (k % 4) + 4) % 4

    def remote(src, dst, ssem, rsem, d, t):
        return pltpu.make_async_remote_copy(
            src_ref=src, dst_ref=dst, send_sem=ssem, recv_sem=rsem, device_id=(d, t), device_id_type=MESH
        )

    def drain(ref, sem):
        pltpu.make_async_copy(ref, ref, sem).wait()

    barrier = pltpu.get_barrier_semaphore()

    def greet(d, t):
        pl.semaphore_signal(barrier, inc=1, device_id=(d, t), device_id_type=MESH)

    def greet_peer(i, carry):
        d = 2 * i + c

        @pl.when(jnp.logical_not(jnp.logical_and(d == dp, to_self)))
        def _():
            greet(d, peer_t)

        return carry

    lax.fori_loop(0, HALF, greet_peer, 0)
    for off in range(1, 8):
        greet(dp, (tp + off) % 8)
    b_right = line(a_me, (b_me + 1) % RING)
    b_left = line(a_me, (b_me + 7) % RING)
    a_right = line((a_me + 1) % RING, b_me)
    a_left = line((a_me + 7) % RING, b_me)
    for d in (a_right, a_left, b_right, b_left):
        greet(d, tp)

    loads = [
        pltpu.make_async_copy(wg_in, wg.at[0], local_sem.at[0]),
        pltpu.make_async_copy(wu_in, wu.at[0], local_sem.at[1]),
        pltpu.make_async_copy(wd_in, wd.at[0], local_sem.at[2]),
        pltpu.make_async_copy(sh_own, shw.at[dp], local_sem.at[3]),
    ]
    for copy in loads[:3]:
        copy.start()
    for n, piece in enumerate((sh_gate, sh_up, sh_down)):
        sh_own[:, n * SPAD : n * SPAD + SHID] = piece[...]
        sh_own[:, n * SPAD + SHID : (n + 1) * SPAD] = jnp.zeros((32, SPAD - SHID), BF16)
    for n in range(WIDTH // 128):
        sgate[:, n * 128 : (n + 1) * 128] = sgate_in[n : n + 1, :].astype(F32)

    place = iota((64, 60), 0)
    slot = 2 * (place % HALF) + place // HALF
    slot_map = jnp.where(slot == emap[...], 1.0, 0.0)
    slot_expert = slot_map.astype(BF16)
    expert = iota((60, TOK), 0)
    named = jnp.zeros((60, TOK), F32)
    for k in range(4):
        named = named + jnp.where(expert == ids[k : k + 1, :], 1.0, 0.0)
    chosen = mm(slot_expert, named.astype(BF16))
    before = one_hot(iota((TOK, TOK), 0) < iota((TOK, TOK), 1))
    rank1 = chosen * (mm(chosen.astype(BF16), before) + 1.0)
    rank1_b = rank1.astype(BF16)
    spread = one_hot(iota((MAIN, 64), 1) == c * HALF + peer_of(iota((MAIN, 64), 0) // 8))
    wide = mm(spread, rank1_b)
    pick_main = one_hot(wide == (iota((MAIN, TOK), 0) % 8 + 1).astype(F32))
    pick_nine = one_hot(wide == float(CAP))
    quarter_cols = pl.ds(pl.multiple_of(x * QUARTER, 128), QUARTER)
    table = jnp.concatenate([tok[:, quarter_cols], cot[:, quarter_cols]], axis=1)
    block, extra = pack(mm(pick_main, table), mm(pick_nine, table))
    send[:, :, : 2 * QUARTER] = block.astype(BF16)
    send[:, :, 2 * QUARTER :] = extra.astype(BF16)

    pl.semaphore_wait(barrier, HALF + 11 - to_self.astype(jnp.int32))

    def a2a(src, dst, ssem, rsem, lo, hi, sign):
        def step(k, carry):
            i = peer_of(k, sign)
            own = jnp.logical_and(k == OWN, to_self)

            @pl.when(own)
            def _():
                pltpu.make_async_copy(src.at[k], dst(k), rsem).start()

            @pl.when(jnp.logical_not(own))
            def _():
                remote(src.at[k], dst(k), ssem, rsem, 2 * i + c, peer_t).start()

            return carry

        lax.fori_loop(lo, hi, step, 0)

    def a2a_sent(src, ssem):
        @pl.when(to_self)
        def _():
            drain(src.at[0 : HALF - 1], ssem)

        @pl.when(jnp.logical_not(to_self))
        def _():
            drain(src, ssem)

    def line_step(k):
        lo, hi = (slice(0, 32), slice(0, 32)) if k < 4 else (slice(0, 16), slice(16, 32))
        at_r = line((a_me + RING - (k - 1)) % RING, b_me)
        at_l = line((a_me + k - 1) % RING, b_me)
        src_r, src_l = (sh_own, sh_own) if k == 1 else (shw.at[at_r], shw.at[at_l])
        remote(src_r.at[lo], shw.at[at_r, lo], pr_send.at[k - 1], pr_recv.at[k - 1], a_right, tp).start()
        remote(src_l.at[hi], shw.at[at_l, hi], pl_send.at[k - 1], pl_recv.at[k - 1], a_left, tp).start()

    def line_wait(k):
        part = shw.at[0] if k < 4 else shw.at[0, 0:16]
        drain(part, pr_recv.at[k - 1])
        drain(part, pl_recv.at[k - 1])

    def dispatch(g):
        a2a(send, lambda k: gat.at[x, k], d_send, d_recv.at[g], 8 * g, 8 * g + 8, 1)

    loads[3].start()
    line_step(1)
    dispatch(0)
    line_wait(1)
    line_step(2)
    dispatch(1)

    w_copies = [
        remote(wg_in, wg.at[1], w_send.at[0], w_recv.at[0], dp, x * 2 + 1 - c),
        remote(wu_in, wu.at[1], w_send.at[1], w_recv.at[1], dp, x * 2 + 1 - c),
        remote(wd_in, wd.at[1], w_send.at[2], w_recv.at[2], dp, x * 2 + 1 - c),
    ]
    for copy in w_copies:
        copy.start()

    router_s = mm(slot_expert, router[...]).astype(BF16)
    logits = nt(router_s, tok[...])
    live = jnp.sum(slot_map, axis=1, keepdims=True) > 0.5
    expd = jnp.where(live, jnp.exp(logits), 0.0)
    prob = expd / jnp.sum(expd, axis=0, keepdims=True)
    gate_w = chosen * prob
    scale = 1.0 / (
        1.0 + jnp.exp(-jnp.sum(tok[...].astype(F32) * sgate[...], axis=1, keepdims=True))
    )

    sent = []

    def go(copy):
        copy.start()
        sent.append(copy)

    def part(g, n):
        return slice(8 * g + 4 * n, 8 * g + 4 * n + 4)

    def x_copy(g, n, q, half, t):
        at = part(g, half)
        return remote(gat.at[q, at], gat.at[q, at], x_send.at[6 * g + n], x_recv.at[6 * g + n], dp, t)

    def x_first(g):
        drain(gat.at[x, 0:8], d_recv.at[g])
        go(x_copy(g, 0, x, 0, right))
        go(x_copy(g, 1, x, 1, left))
        go(x_copy(g, 2, x, 1, right))
        go(x_copy(g, 3, x, 0, left))

    def x_forward(g):
        x_copy(g, 0, x3, 0, left).wait_recv()
        go(x_copy(g, 4, x3, 0, right))
        x_copy(g, 1, x1, 1, right).wait_recv()
        go(x_copy(g, 5, x1, 1, left))

    def feed(q, start):
        unpack_into(xrow, gat[q])
        at = pl.ds(pl.multiple_of(q * QUARTER, 128), QUARTER)
        for p in range(2):
            parts = (
                nt(xrow[:, :QUARTER], wg[p, :, at]),
                nt(xrow[:, :QUARTER], wu[p, :, at]),
                nt(xrow[:, QUARTER:], wd[p, :, at]),
            )
            for n, part in enumerate(parts):
                if start:
                    acc[3 * p + n] = part
                else:
                    acc[3 * p + n] += part

    def line_send(b, half, ssem, rsem, target):
        for off in ((2, 5, 3, 4) if half else (0, 7, 1, 6)):
            at_ = line((a_me + off) % RING, b % RING)
            remote(shw.at[at_], shw.at[at_], ssem, rsem, target, tp).start()

    def ring_step(k, half):
        n = 2 * (k - 1) + half
        if k > 1:
            drain(shw.at[0:4], ra_recv.at[n - 2])
            drain(shw.at[0:4], la_recv.at[n - 2])
        if k < 4 or half == 0:
            line_send(b_me + RING - (k - 1), half, ra_send.at[n], ra_recv.at[n], b_right)
        if k < 4 or half == 1:
            line_send(b_me + (k - 1), half, la_send.at[n], la_recv.at[n], b_left)

    line_wait(2)
    line_step(3)
    dispatch(2)
    x_first(0)
    line_wait(3)
    line_step(4)
    dispatch(3)
    loads[3].wait()
    ring_step(1, 0)
    x_forward(0)
    x_first(1)
    line_wait(4)
    ring_step(1, 1)
    x_forward(1)
    x_first(2)
    ring_step(2, 0)
    x_forward(2)
    for copy in loads[:3]:
        copy.wait()
    for copy in w_copies:
        copy.wait_recv()
    x_first(3)
    ring_step(2, 1)
    feed(x, True)
    x_forward(3)
    ring_step(3, 0)
    for g in range(SETS):
        x_copy(g, 2, x3, 1, left).wait_recv()
    feed(x3, False)
    for g in range(SETS):
        x_copy(g, 3, x1, 0, right).wait_recv()
    feed(x1, False)
    ring_step(3, 1)
    for g in range(SETS):
        x_copy(g, 4, x2, 0, left).wait_recv()
        x_copy(g, 5, x2, 1, right).wait_recv()
    feed(x2, False)

    row_dots = jnp.zeros((ROWS, 1), F32)
    for p in range(2):
        active, slope = silu_pair(acc[3 * p])
        up, grad_hidden = acc[3 * p + 1], acc[3 * p + 2]
        hid[p] = (active * up).astype(BF16)
        gg[p] = (grad_hidden * up * slope).astype(BF16)
        gu[p] = (grad_hidden * active).astype(BF16)
        row_dots = row_dots + jnp.sum(hid[p].astype(F32) * grad_hidden, axis=1, keepdims=True)

    repeat = one_hot(iota((MAIN, HALF), 1) == iota((MAIN, HALF), 0) // 8)

    def produce(q):
        at = pl.ds(pl.multiple_of(q * QUARTER, 128), QUARTER)
        out = mm(hid[0], wd[0, :, at]) + mm(hid[1], wd[1, :, at])
        grad = mm(gg[0], wg[0, :, at]) + mm(gg[1], wg[1, :, at])
        grad = grad + mm(gu[0], wu[0, :, at]) + mm(gu[1], wu[1, :, at])
        both = jnp.concatenate([out, grad], axis=1)
        return pack(both[:MAIN], mm(repeat, both[MAIN:].astype(BF16)))

    def put(ref, packed):
        ref[:, :, : 2 * QUARTER] = packed[0].astype(BF16)
        ref[:, :, 2 * QUARTER :] = packed[1].astype(BF16)

    def add_part(ref, at, more):
        ref[at] = (ref[at].astype(F32) + more.astype(F32)).astype(BF16)

    def rs_copy(g, n):
        at = part(g, n % 2)
        src, dst, t = (
            (outs.at[0, at], rs_a.at[g], right),
            (outs.at[0, at], rs_b.at[g], left),
            (outs.at[1, part(g, 1)], rs_l.at[part(g, 1)], right),
            (outs.at[2, part(g, 0)], rs_r.at[part(g, 0)], left),
            (outs.at[1, at], rs_l.at[at], right),
            (outs.at[2, at], rs_r.at[at], left),
        )[n]
        return remote(src, dst, rs_send.at[6 * g + n], rs_recv.at[6 * g + n], dp, t)

    def rs_start(g):
        go(rs_copy(g, 0))
        go(rs_copy(g, 1))

    def rs_free(g):
        go(rs_copy(g, 2))
        go(rs_copy(g, 3))

    def rs_forward(g):
        rs_copy(g, 0).wait_recv()
        add_part(outs, (1, part(g, 0)), rs_a[g])
        go(rs_copy(g, 4))
        rs_copy(g, 1).wait_recv()
        add_part(outs, (2, part(g, 1)), rs_b[g])
        go(rs_copy(g, 5))

    def give_back(g):
        for n in range(2, 6):
            rs_copy(g, n).wait_recv()
        at = slice(8 * g, 8 * g + 8)
        add_part(ret_s, at, rs_l[at].astype(F32) + rs_r[at].astype(F32))
        a2a(ret_s, lambda k: ret_r.at[k], t_send, t_recv.at[g], 8 * g, 8 * g + 8, -1)

    put(outs.at[0], produce(x2))
    rs_start(0)
    ring_step(4, 0)
    put(outs.at[1], produce(x1))
    go(rs_copy(0, 2))
    put(outs.at[2], produce(x3))
    go(rs_copy(0, 3))
    rs_start(1)
    ring_step(4, 1)

    n_high, n_low = halves(jnp.broadcast_to(row_dots[MAIN:], (HALF, 128)))
    m_high, m_low = halves(jnp.broadcast_to(row_dots[:MAIN], (MAIN, 128)))
    lane = iota((MAIN, 128), 1) // 32
    both_dots = jnp.where(lane == 2, mm(repeat, n_high), mm(repeat, n_low))
    both_dots = jnp.where(lane == 0, m_high.astype(F32), jnp.where(lane == 1, m_low.astype(F32), both_dots))
    dot_s[...] = both_dots.reshape(HALF, 8, 128).astype(BF16)
    put(ret_s, produce(x))
    a2a(dot_s, lambda k: dot_r.at[k], o_send, o_recv, 0, HALF, -1)

    rs_forward(0)
    rs_free(1)
    rs_start(2)
    rs_forward(1)
    rs_free(2)
    rs_start(3)
    rs_forward(2)
    rs_free(3)

    drain(shw.at[0:4], ra_recv.at[6])
    drain(shw.at[0:4], la_recv.at[7])
    give_back(0)
    give_back(1)

    own_slot = peer_of(iota((HALF, MAIN), 1) // 8) == iota((HALF, MAIN), 0)
    gather_main = one_hot(own_slot)
    gather_nine = one_hot(jnp.logical_and(own_slot, iota((HALF, MAIN), 1) % 8 == 0))
    drain(dot_r, o_recv)
    flat_dots = dot_r[...].astype(F32).reshape(MAIN, 128)
    p_high, p_low = halves(pick_main.astype(F32) * (flat_dots[:, 0:1] + flat_dots[:, 32:33]))
    n_high, n_low = halves(pick_nine.astype(F32) * (flat_dots[:, 64:65] + flat_dots[:, 96:97]))
    dx_s[...] = (
        mm(gather_main, p_high) + mm(gather_main, p_low) + mm(gather_nine, n_high) + mm(gather_nine, n_low)
    )
    dx_r[tp] = dx_s[...]
    for off in range(1, 8):
        remote(dx_s, dx_r.at[tp], dx_send, dx_recv, dp, (tp + off) % 8).start()

    def shared_in(n, carry):
        cols = pl.ds(pl.multiple_of(n * QUARTER, 128), QUARTER)
        blocks = pl.ds(n * 16, 16)
        parts = (
            mm(tok[:, cols], shw[blocks, :, 0:SHID].reshape(QUARTER, SHID)),
            mm(tok[:, cols], shw[blocks, :, SPAD : SPAD + SHID].reshape(QUARTER, SHID)),
            mm(cot[:, cols], shw[blocks, :, 2 * SPAD : 2 * SPAD + SHID].reshape(QUARTER, SHID)),
        )
        for m, part in enumerate(parts):
            sh_acc[m] = part + jnp.where(n == 0, 0.0, 1.0) * sh_acc[m]
        return carry

    for m in range(3):
        sh_acc[m] = jnp.zeros((TOK, SHID), F32)
    lax.fori_loop(0, XS, shared_in, 0)
    active, slope = silu_pair(sh_acc[0])
    sh_grad = sh_acc[2]
    sh_hid = (active * sh_acc[1]).astype(BF16)
    sh_gg = (sh_grad * sh_acc[1] * slope).astype(BF16)
    sh_gu = (sh_grad * active).astype(BF16)
    dot_high, dot_low = halves(sh_hid.astype(F32) * sh_grad)
    ones_s = jnp.ones((8, SHID), BF16)
    sx_s[...] = nt(ones_s, dot_high) + nt(ones_s, dot_low)
    sx_r[tp] = sx_s[...]
    for off in range(1, 8):
        remote(sx_s, sx_r.at[tp], sx_send, sx_recv, dp, (tp + off) % 8).start()

    rs_forward(3)
    give_back(2)

    def shared_out(q):
        blocks = pl.ds(q * 16, 16)
        out = nt(sh_hid, shw[blocks, :, 2 * SPAD : 2 * SPAD + SHID].reshape(QUARTER, SHID))
        grad = nt(sh_gg, shw[blocks, :, 0:SHID].reshape(QUARTER, SHID))
        grad = grad + nt(sh_gu, shw[blocks, :, SPAD : SPAD + SHID].reshape(QUARTER, SHID))
        return jnp.concatenate([out * scale, grad * scale], axis=1)

    def s_copy(n, src, dst, t):
        return remote(src, dst, s_send.at[n], s_recv.at[n], dp, t)

    top, low_ = slice(0, 64), slice(64, TOK)
    sh_s[0] = shared_out(x2).astype(BF16)
    go(s_copy(0, sh_s.at[0, top], sh_r.at[0, top], right))
    go(s_copy(1, sh_s.at[0, low_], sh_r.at[0, low_], left))
    sh_s[1] = shared_out(x1).astype(BF16)
    go(s_copy(2, sh_s.at[1, low_], sh_r.at[1, low_], right))
    sh_s[2] = shared_out(x3).astype(BF16)
    go(s_copy(3, sh_s.at[2, top], sh_r.at[2, top], left))

    give_back(3)
    total = shared_out(x)

    s_copy(0, sh_s.at[0, top], sh_r.at[0, top], left).wait_recv()
    add_part(sh_s, (1, top), sh_r[0, top])
    go(s_copy(4, sh_s.at[1, top], sh_r.at[1, top], right))
    s_copy(1, sh_s.at[0, low_], sh_r.at[0, low_], right).wait_recv()
    add_part(sh_s, (2, low_), sh_r[0, low_])
    go(s_copy(5, sh_s.at[2, low_], sh_r.at[2, low_], left))

    rank_t = rank1.T.astype(BF16)
    w_high, w_low = halves(gate_w.T)
    wide_t = nt(rank_t, spread)
    gate_t = nt(w_high, spread) + nt(w_low, spread)
    weigh_main = jnp.where(wide_t == (iota((TOK, MAIN), 1) % 8 + 1).astype(F32), gate_t, 0.0)
    spread9 = one_hot(iota((HALF, 64), 1) == c * HALF + peer_of(iota((HALF, 64), 0)))
    wide9_t = nt(rank_t, spread9)
    gate9_t = nt(w_high, spread9) + nt(w_low, spread9)
    weigh_nine = jnp.where(wide9_t == float(CAP), gate9_t, 0.0)
    main_high, main_low = halves(weigh_main)
    nine_high, nine_low = halves(weigh_nine)

    drain(dx_r.at[0:7], dx_recv)
    even = dx_r[0] + dx_r[2] + dx_r[4] + dx_r[6]
    odd = dx_r[1] + dx_r[3] + dx_r[5] + dx_r[7]
    slot_dots = jnp.concatenate([even, odd], axis=0)
    drain(sx_r.at[0:7], sx_recv)
    sh_dots = jnp.sum(sx_r[...], axis=0).T[:, 0:1]
    taken = chosen * slot_dots
    dlogits = prob * (taken - jnp.sum(gate_w * slot_dots, axis=0, keepdims=True))
    l_high, l_low = halves(dlogits.T)
    router_q = mm(slot_expert, router[:, pl.ds(pl.multiple_of(tp * EIGHTH, 128), EIGHTH)]).astype(BF16)
    grad = mm(l_high, router_q) + mm(l_low, router_q)
    sg_cols = sgate[:, pl.ds(pl.multiple_of(tp * EIGHTH, 128), EIGHTH)]
    grad = grad + sh_dots * scale * (1.0 - scale) * sg_cols

    s_copy(2, sh_s.at[1, low_], sh_r.at[1, low_], left).wait_recv()
    s_copy(3, sh_s.at[2, top], sh_r.at[2, top], right).wait_recv()
    s_copy(4, sh_s.at[1, top], sh_r.at[1, top], left).wait_recv()
    s_copy(5, sh_s.at[2, low_], sh_r.at[2, low_], right).wait_recv()
    total = total + sh_r[1].astype(F32) + sh_r[2].astype(F32)

    for g in range(SETS):
        drain(ret_r.at[0:8], t_recv.at[g])
    unpack_into(xrow, ret_r[...])
    total = total + mm(main_high, xrow[0:MAIN, :]) + mm(main_low, xrow[0:MAIN, :])
    total = total + mm(nine_high, xrow[MAIN:ROWS, :]) + mm(nine_low, xrow[MAIN:ROWS, :])
    low = jnp.concatenate([total[:, 0:EIGHTH], total[:, QUARTER : QUARTER + EIGHTH]], axis=1)
    high = jnp.concatenate([total[:, EIGHTH:QUARTER], total[:, QUARTER + EIGHTH :]], axis=1)
    px_s[...] = jnp.where(c == 0, high, low)
    own = jnp.where(c == 0, low, high)
    px = remote(px_s, px_r, px_sem.at[0], px_sem.at[1], dp, x * 2 + 1 - c)
    px.start()
    px.wait_recv()
    both = own + px_r[...]
    result[:, :EIGHTH] = both[:, :EIGHTH]
    result[:, EIGHTH:] = both[:, EIGHTH:] + grad

    a2a_sent(send, d_send)
    a2a_sent(ret_s, t_send)
    a2a_sent(dot_s, o_send)
    for copy in (*w_copies, *sent, px):
        copy.wait_send()
    for k in range(4):
        part = shw.at[0] if k < 3 else shw.at[0, 0:16]
        drain(part, pr_send.at[k])
        drain(part, pl_send.at[k])
    for n in range(7):
        drain(shw.at[0:4], ra_send.at[n])
        drain(shw.at[0:4], la_send.at[n if n < 6 else 7])
    drain(dx_r.at[0:7], dx_send)
    drain(sx_r.at[0:7], sx_send)


def shards(
    tokens, grad_out, route_ids, expert_map, router, shared_gate, sh_gate, sh_up, sh_down, ex_gate, ex_up, ex_down
):
    vmem = pl.BlockSpec(memory_space=pltpu.VMEM)
    hbm = pl.BlockSpec(memory_space=pl.ANY)
    dma = pltpu.SemaphoreType.DMA
    block = (HALF, 8, PACK)
    sums = pl.pallas_call(
        body,
        out_shape=jax.ShapeDtypeStruct((TOK, QUARTER), F32),
        in_specs=[vmem] * 9 + [hbm] * 3,
        out_specs=vmem,
        scratch_shapes=[
            pltpu.VMEM(block, BF16),
            pltpu.VMEM((XS, *block), BF16),
            pltpu.VMEM((2, HID, WIDTH), BF16),
            pltpu.VMEM((2, HID, WIDTH), BF16),
            pltpu.VMEM((2, HID, WIDTH), BF16),
            pltpu.VMEM((ROWS, 2 * QUARTER), BF16),
            pltpu.VMEM((6, ROWS, HID), F32),
            pltpu.VMEM((2, ROWS, HID), BF16),
            pltpu.VMEM((2, ROWS, HID), BF16),
            pltpu.VMEM((2, ROWS, HID), BF16),
            pltpu.VMEM((3, *block), BF16),
            pltpu.VMEM((SETS, 4, 8, PACK), BF16),
            pltpu.VMEM((SETS, 4, 8, PACK), BF16),
            pltpu.VMEM(block, BF16),
            pltpu.VMEM(block, BF16),
            pltpu.VMEM(block, BF16),
            pltpu.VMEM(block, BF16),
            pltpu.VMEM((RING * RING, 32, 3 * SPAD), BF16),
            pltpu.VMEM((32, 3 * SPAD), BF16),
            pltpu.VMEM((1, WIDTH), F32),
            pltpu.VMEM((3, TOK, 2 * QUARTER), BF16),
            pltpu.VMEM((3, TOK, 2 * QUARTER), BF16),
            pltpu.VMEM((TOK, QUARTER), F32),
            pltpu.VMEM((TOK, QUARTER), F32),
            pltpu.VMEM((HALF, TOK), F32),
            pltpu.VMEM((8, HALF, TOK), F32),
            pltpu.VMEM((3, TOK, SHID), F32),
            pltpu.VMEM((HALF, 8, 128), BF16),
            pltpu.VMEM((HALF, 8, 128), BF16),
            pltpu.VMEM((8, TOK), F32),
            pltpu.VMEM((8, 8, TOK), F32),
            dma((4,)), dma((3,)), dma((3,)), dma, dma((4,)), dma((24,)), dma((24,)), dma((24,)), dma((24,)),
            dma, dma((4,)), dma((4,)), dma((4,)), dma((4,)), dma((4,)), dma((8,)), dma((8,)), dma((8,)), dma((8,)),
            dma((6,)), dma((6,)), dma((2,)), dma, dma, dma, dma, dma, dma,
        ],
        compiler_params=pltpu.CompilerParams(
            collective_id=0, has_side_effects=True, vmem_limit_bytes=60 * 1024 * 1024
        ),
    )(
        tokens, grad_out, route_ids.T, expert_map.reshape(1, 60), router.T, shared_gate.reshape(16, 128),
        sh_gate, sh_up, sh_down.T,
        ex_gate.reshape(WIDTH, HID).T, ex_up.reshape(WIDTH, HID).T, ex_down.reshape(HID, WIDTH),
    )
    return sums[:, :EIGHTH].astype(BF16), sums[:, EIGHTH:].astype(BF16)


def solution(mesh):
    placed = (
        P("dp", None), P("dp", None), P("dp", None), P(), P(), P(),
        P("dp", "tensor"), P("dp", "tensor"), P("tensor", "dp"),
        P("dp", None, "tensor"), P("dp", None, "tensor"), P("dp", "tensor", None),
    )
    return jax.shard_map(
        shards,
        mesh=mesh,
        in_specs=placed,
        out_specs=(P("dp", "tensor"), P("dp", "tensor")),
        check_vma=False,
    )
```

```python
import jax
import jax.numpy as jnp
from jax import lax
from jax.experimental import pallas as pl
from jax.experimental.pallas import tpu as pltpu
from jax.sharding import PartitionSpec as P

MESH = pl.DeviceIdType.MESH
F32 = jnp.float32
BF16 = jnp.bfloat16
RING = 8
XS = 4
CAP = 9
HALF = 32
TOK = 128
WIDTH = 2048
QUARTER = WIDTH // XS
EIGHTH = QUARTER // 2
PACK = 2 * QUARTER + 128
HID = 176
SHID = 352
SPAD = 384
MAIN = HALF * 8
OWN = 16
SETS = 4
ROWS = HALF * CAP


def mm(a, b):
    return jnp.dot(a, b, preferred_element_type=F32)


def nt(a, b):
    return lax.dot_general(a, b, (((1,), (1,)), ((), ())), preferred_element_type=F32)


def halves(v):
    high = v.astype(BF16)
    return high, (v - high.astype(F32)).astype(BF16)


def silu_pair(v):
    s = 1.0 / (1.0 + jnp.exp(-v))
    return v * s, s * (1.0 + v * (1.0 - s))


def iota(shape, dim):
    return lax.broadcasted_iota(jnp.int32, shape, dim)


def one_hot(mask):
    return jnp.where(mask, 1.0, 0.0).astype(BF16)


def unpack_into(rows_ref, blocks):
    flat = blocks.astype(F32).reshape(MAIN, PACK)
    rows_ref[0:MAIN, :] = flat[:, : 2 * QUARTER].astype(BF16)
    extra = flat[:, 2 * QUARTER :].astype(BF16)
    row, col = iota((HALF, MAIN), 0), iota((HALF, MAIN), 1)
    for q in range(8):
        ninth = mm(one_hot(col == row * 8 + q), extra)
        rows_ref[MAIN:ROWS, q * 128 : (q + 1) * 128] = ninth.astype(BF16)


def pack(main, ninth):
    sub = iota((MAIN, 128), 0) % 8
    extra = jnp.zeros((MAIN, 128), F32)
    for q in range(8):
        extra = jnp.where(sub == q, ninth[:, q * 128 : (q + 1) * 128], extra)
    return main.reshape(HALF, 8, 2 * QUARTER), extra.reshape(HALF, 8, 128)


def body(
    tok, cot, ids, emap, router, sgate_in, sh_gate, sh_up, sh_down, wg_in, wu_in, wd_in,
    result,
    send, gat, wg, wu, wd, xrow, acc, hid, gg, gu, outs, rs_a, rs_b, rs_l, rs_r,
    ret_s, ret_r, shw, sh_own, sgate, sh_s, sh_r, keep, ps_s, ps_r, px_s, px_r, dx_s, dx_r, sh_acc, dot_s, dot_r, sx_s, sx_r,
    local_sem, w_send, w_recv, d_send, d_recv, x_send, x_recv, rs_send, rs_recv,
    t_send, t_recv, pr_send, pr_recv, pl_send, pl_recv, ra_send, ra_recv, la_send, la_recv,
    s_send, s_recv, px_sem, dx_send, dx_recv, o_send, o_recv, sx_send, sx_recv, ps_send, ps_recv,
):
    dp = lax.axis_index("dp")
    tp = lax.axis_index("tensor")
    x, c = tp // 2, tp % 2
    mine = dp // 2
    parity = dp % 2
    peer_t = x * 2 + parity
    to_self = parity == c
    right = ((x + 1) % XS) * 2 + c
    left = ((x + XS - 1) % XS) * 2 + c
    opposite = ((x + 2) % XS) * 2 + c
    x1, x2, x3 = (x + 1) % XS, (x + 2) % XS, (x + 3) % XS
    zc, yc = dp // RING, dp % RING
    a_me = jnp.where(c == 0, yc, zc)
    b_me = jnp.where(c == 0, zc, yc)

    def line(a, b):
        return a * (1 + 7 * c) + b * (8 - 7 * c)

    def peer_of(k, sign=1):
        j = k // 4
        dz = jnp.where(j < 2, 1 + 4 * j, jnp.where(j < 4, 15 - 4 * j, jnp.where(j < 6, 4 * j - 16, 4 * j - 22)))
        return ((zc + sign * dz + RING) % RING) * 4 + (yc // 2 + sign * (k % 4) + 4) % 4

    def remote(src, dst, ssem, rsem, d, t):
        return pltpu.make_async_remote_copy(
            src_ref=src, dst_ref=dst, send_sem=ssem, recv_sem=rsem, device_id=(d, t), device_id_type=MESH
        )

    def drain(ref, sem):
        pltpu.make_async_copy(ref, ref, sem).wait()

    barrier = pltpu.get_barrier_semaphore()

    def greet(d, t):
        pl.semaphore_signal(barrier, inc=1, device_id=(d, t), device_id_type=MESH)

    def greet_peer(i, carry):
        d = 2 * i + c

        @pl.when(jnp.logical_not(jnp.logical_and(d == dp, to_self)))
        def _():
            greet(d, peer_t)

        return carry

    lax.fori_loop(0, HALF, greet_peer, 0)
    for off in range(1, 8):
        greet(dp, (tp + off) % 8)
    b_right = line(a_me, (b_me + 1) % RING)
    b_left = line(a_me, (b_me + 7) % RING)
    a_right = line((a_me + 1) % RING, b_me)
    a_left = line((a_me + 7) % RING, b_me)
    for d in (a_right, a_left, b_right, b_left):
        greet(d, tp)

    loads = [
        pltpu.make_async_copy(wg_in, wg.at[0], local_sem.at[0]),
        pltpu.make_async_copy(wu_in, wu.at[0], local_sem.at[1]),
        pltpu.make_async_copy(wd_in, wd.at[0], local_sem.at[2]),
        pltpu.make_async_copy(sh_own, shw.at[dp], local_sem.at[3]),
    ]
    for copy in loads[:3]:
        copy.start()
    for n, piece in enumerate((sh_gate, sh_up, sh_down)):
        sh_own[:, n * SPAD : n * SPAD + SHID] = piece[...]
        sh_own[:, n * SPAD + SHID : (n + 1) * SPAD] = jnp.zeros((32, SPAD - SHID), BF16)
    for n in range(WIDTH // 128):
        sgate[:, n * 128 : (n + 1) * 128] = sgate_in[n : n + 1, :].astype(F32)

    place = iota((64, 60), 0)
    slot = 2 * (place % HALF) + place // HALF
    slot_map = jnp.where(slot == emap[...], 1.0, 0.0)
    slot_expert = slot_map.astype(BF16)
    expert = iota((60, TOK), 0)
    named = jnp.zeros((60, TOK), F32)
    for k in range(4):
        named = named + jnp.where(expert == ids[k : k + 1, :], 1.0, 0.0)
    chosen = mm(slot_expert, named.astype(BF16))
    before = one_hot(iota((TOK, TOK), 0) < iota((TOK, TOK), 1))
    rank1 = chosen * (mm(chosen.astype(BF16), before) + 1.0)
    rank1_b = rank1.astype(BF16)
    spread = one_hot(iota((MAIN, 64), 1) == c * HALF + peer_of(iota((MAIN, 64), 0) // 8))
    wide = mm(spread, rank1_b)
    pick_main = one_hot(wide == (iota((MAIN, TOK), 0) % 8 + 1).astype(F32))
    pick_nine = one_hot(wide == float(CAP))
    quarter_cols = pl.ds(pl.multiple_of(x * QUARTER, 128), QUARTER)
    table = jnp.concatenate([tok[:, quarter_cols], cot[:, quarter_cols]], axis=1)
    block, extra = pack(mm(pick_main, table), mm(pick_nine, table))
    send[:, :, : 2 * QUARTER] = block.astype(BF16)
    send[:, :, 2 * QUARTER :] = extra.astype(BF16)

    pl.semaphore_wait(barrier, HALF + 11 - to_self.astype(jnp.int32))

    def a2a(src, dst, ssem, rsem, lo, hi, sign):
        def step(k, carry):
            i = peer_of(k, sign)
            own = jnp.logical_and(k == OWN, to_self)

            @pl.when(own)
            def _():
                pltpu.make_async_copy(src.at[k], dst(k), rsem).start()

            @pl.when(jnp.logical_not(own))
            def _():
                remote(src.at[k], dst(k), ssem, rsem, 2 * i + c, peer_t).start()

            return carry

        lax.fori_loop(lo, hi, step, 0)

    def a2a_sent(src, ssem):
        @pl.when(to_self)
        def _():
            drain(src.at[0 : HALF - 1], ssem)

        @pl.when(jnp.logical_not(to_self))
        def _():
            drain(src, ssem)

    def line_step(k):
        lo, hi = (slice(0, 32), slice(0, 32)) if k < 4 else (slice(0, 16), slice(16, 32))
        at_r = line((a_me + RING - (k - 1)) % RING, b_me)
        at_l = line((a_me + k - 1) % RING, b_me)
        src_r, src_l = (sh_own, sh_own) if k == 1 else (shw.at[at_r], shw.at[at_l])
        remote(src_r.at[lo], shw.at[at_r, lo], pr_send.at[k - 1], pr_recv.at[k - 1], a_right, tp).start()
        remote(src_l.at[hi], shw.at[at_l, hi], pl_send.at[k - 1], pl_recv.at[k - 1], a_left, tp).start()

    def line_wait(k):
        part = shw.at[0] if k < 4 else shw.at[0, 0:16]
        drain(part, pr_recv.at[k - 1])
        drain(part, pl_recv.at[k - 1])

    def dispatch(g):
        a2a(send, lambda k: gat.at[x, k], d_send, d_recv.at[g], 8 * g, 8 * g + 8, 1)

    loads[3].start()
    line_step(1)
    dispatch(0)
    line_wait(1)
    line_step(2)
    dispatch(1)

    w_copies = [
        remote(wg_in, wg.at[1], w_send.at[0], w_recv.at[0], dp, x * 2 + 1 - c),
        remote(wu_in, wu.at[1], w_send.at[1], w_recv.at[1], dp, x * 2 + 1 - c),
        remote(wd_in, wd.at[1], w_send.at[2], w_recv.at[2], dp, x * 2 + 1 - c),
    ]
    for copy in w_copies:
        copy.start()

    router_s = mm(slot_expert, router[...]).astype(BF16)
    logits = nt(router_s, tok[...])
    live = jnp.sum(slot_map, axis=1, keepdims=True) > 0.5
    expd = jnp.where(live, jnp.exp(logits), 0.0)
    prob = expd / jnp.sum(expd, axis=0, keepdims=True)
    gate_w = chosen * prob
    scale = 1.0 / (
        1.0 + jnp.exp(-jnp.sum(tok[...].astype(F32) * sgate[...], axis=1, keepdims=True))
    )

    sent = []

    def go(copy):
        copy.start()
        sent.append(copy)

    def part(g, n):
        return slice(8 * g + 4 * n, 8 * g + 4 * n + 4)

    def x_copy(g, n, q, half, t):
        at = part(g, half)
        return remote(gat.at[q, at], gat.at[q, at], x_send.at[6 * g + n], x_recv.at[6 * g + n], dp, t)

    def x_first(g):
        drain(gat.at[x, 0:8], d_recv.at[g])
        go(x_copy(g, 0, x, 0, right))
        go(x_copy(g, 1, x, 1, left))
        go(x_copy(g, 2, x, 1, right))
        go(x_copy(g, 3, x, 0, left))

    def x_forward(g):
        x_copy(g, 0, x3, 0, left).wait_recv()
        go(x_copy(g, 4, x3, 0, right))
        x_copy(g, 1, x1, 1, right).wait_recv()
        go(x_copy(g, 5, x1, 1, left))

    def feed(q, start):
        unpack_into(xrow, gat[q])
        at = pl.ds(pl.multiple_of(q * QUARTER, 128), QUARTER)
        for p in range(2):
            parts = (
                nt(xrow[:, :QUARTER], wg[p, :, at]),
                nt(xrow[:, :QUARTER], wu[p, :, at]),
                nt(xrow[:, QUARTER:], wd[p, :, at]),
            )
            for n, part in enumerate(parts):
                if start:
                    acc[3 * p + n] = part
                else:
                    acc[3 * p + n] += part

    def line_send(b, half, ssem, rsem, target):
        for off in ((2, 5, 3, 4) if half else (0, 7, 1, 6)):
            at_ = line((a_me + off) % RING, b % RING)
            remote(shw.at[at_], shw.at[at_], ssem, rsem, target, tp).start()

    def ring_step(k, half):
        n = 2 * (k - 1) + half
        if k > 1:
            drain(shw.at[0:4], ra_recv.at[n - 2])
            drain(shw.at[0:4], la_recv.at[n - 2])
        if k < 4 or half == 0:
            line_send(b_me + RING - (k - 1), half, ra_send.at[n], ra_recv.at[n], b_right)
        if k < 4 or half == 1:
            line_send(b_me + (k - 1), half, la_send.at[n], la_recv.at[n], b_left)

    line_wait(2)
    line_step(3)
    dispatch(2)
    x_first(0)
    line_wait(3)
    line_step(4)
    dispatch(3)
    loads[3].wait()
    ring_step(1, 0)
    x_forward(0)
    x_first(1)
    line_wait(4)
    ring_step(1, 1)
    x_first(2)
    x_forward(1)
    ring_step(2, 0)
    for copy in loads[:3]:
        copy.wait()
    for copy in w_copies:
        copy.wait_recv()
    x_first(3)
    x_forward(2)
    ring_step(2, 1)
    feed(x, True)
    x_forward(3)
    ring_step(3, 0)
    for g in range(SETS):
        x_copy(g, 2, x3, 1, left).wait_recv()
    feed(x3, False)
    for g in range(SETS):
        x_copy(g, 3, x1, 0, right).wait_recv()
    feed(x1, False)
    ring_step(3, 1)
    for g in range(SETS):
        x_copy(g, 4, x2, 0, left).wait_recv()
        x_copy(g, 5, x2, 1, right).wait_recv()
    feed(x2, False)

    for p in range(2):
        active, slope = silu_pair(acc[3 * p])
        up, grad_hidden = acc[3 * p + 1], acc[3 * p + 2]
        hid[p] = (active * up).astype(BF16)
        gg[p] = (grad_hidden * up * slope).astype(BF16)
        gu[p] = (grad_hidden * active).astype(BF16)

    repeat = one_hot(iota((MAIN, HALF), 1) == iota((MAIN, HALF), 0) // 8)

    def produce(q):
        at = pl.ds(pl.multiple_of(q * QUARTER, 128), QUARTER)
        out = mm(hid[0], wd[0, :, at]) + mm(hid[1], wd[1, :, at])
        grad = mm(gg[0], wg[0, :, at]) + mm(gg[1], wg[1, :, at])
        grad = grad + mm(gu[0], wu[0, :, at]) + mm(gu[1], wu[1, :, at])
        both = jnp.concatenate([out, grad], axis=1)
        return pack(both[:MAIN], mm(repeat, both[MAIN:].astype(BF16)))

    def put(ref, packed):
        ref[:, :, : 2 * QUARTER] = packed[0].astype(BF16)
        ref[:, :, 2 * QUARTER :] = packed[1].astype(BF16)

    def add_part(ref, at, more):
        ref[at] = (ref[at].astype(F32) + more.astype(F32)).astype(BF16)

    def rs_copy(g, n):
        at = part(g, n % 2)
        src, dst, t = (
            (outs.at[0, at], rs_a.at[g], right),
            (outs.at[0, at], rs_b.at[g], left),
            (outs.at[1, part(g, 1)], rs_l.at[part(g, 1)], right),
            (outs.at[2, part(g, 0)], rs_r.at[part(g, 0)], left),
            (outs.at[1, at], rs_l.at[at], right),
            (outs.at[2, at], rs_r.at[at], left),
        )[n]
        return remote(src, dst, rs_send.at[6 * g + n], rs_recv.at[6 * g + n], dp, t)

    def rs_start(g):
        go(rs_copy(g, 0))
        go(rs_copy(g, 1))

    def rs_free(g):
        go(rs_copy(g, 2))
        go(rs_copy(g, 3))

    def rs_forward(g):
        rs_copy(g, 0).wait_recv()
        add_part(outs, (1, part(g, 0)), rs_a[g])
        go(rs_copy(g, 4))
        rs_copy(g, 1).wait_recv()
        add_part(outs, (2, part(g, 1)), rs_b[g])
        go(rs_copy(g, 5))

    def give_back(g):
        for n in range(2, 6):
            rs_copy(g, n).wait_recv()
        at = slice(8 * g, 8 * g + 8)
        add_part(ret_s, at, rs_l[at].astype(F32) + rs_r[at].astype(F32))
        a2a(ret_s, lambda k: ret_r.at[k], t_send, t_recv.at[g], 8 * g, 8 * g + 8, -1)

    put(outs.at[0], produce(x2))
    rs_start(0)
    ring_step(4, 0)
    put(outs.at[1], produce(x1))
    go(rs_copy(0, 2))
    put(outs.at[2], produce(x3))
    go(rs_copy(0, 3))
    rs_start(1)
    ring_step(4, 1)

    rs_forward(0)
    rs_free(1)
    rs_start(2)

    row_dots = jnp.sum(hid[0].astype(F32) * acc[2] + hid[1].astype(F32) * acc[5], axis=1, keepdims=True)
    n_high, n_low = halves(jnp.broadcast_to(row_dots[MAIN:], (HALF, 128)))
    m_high, m_low = halves(jnp.broadcast_to(row_dots[:MAIN], (MAIN, 128)))
    lane = iota((MAIN, 128), 1) // 32
    both_dots = jnp.where(lane == 2, mm(repeat, n_high), mm(repeat, n_low))
    both_dots = jnp.where(lane == 0, m_high.astype(F32), jnp.where(lane == 1, m_low.astype(F32), both_dots))
    dot_s[...] = both_dots.reshape(HALF, 8, 128).astype(BF16)
    put(ret_s, produce(x))
    a2a(dot_s, lambda k: dot_r.at[k], o_send, o_recv, 0, HALF, -1)

    rs_forward(1)
    rs_free(2)
    rs_start(3)

    drain(shw.at[0:4], ra_recv.at[6])
    drain(shw.at[0:4], la_recv.at[7])
    give_back(0)
    rs_forward(2)
    rs_free(3)
    give_back(1)

    own_slot = peer_of(iota((HALF, MAIN), 1) // 8) == iota((HALF, MAIN), 0)
    gather_main = one_hot(own_slot)
    gather_nine = one_hot(jnp.logical_and(own_slot, iota((HALF, MAIN), 1) % 8 == 0))
    drain(dot_r, o_recv)
    flat_dots = dot_r[...].astype(F32).reshape(MAIN, 128)
    p_high, p_low = halves(pick_main.astype(F32) * (flat_dots[:, 0:1] + flat_dots[:, 32:33]))
    n_high, n_low = halves(pick_nine.astype(F32) * (flat_dots[:, 64:65] + flat_dots[:, 96:97]))
    dx_s[...] = (
        mm(gather_main, p_high) + mm(gather_main, p_low) + mm(gather_nine, n_high) + mm(gather_nine, n_low)
    )
    dx_r[tp] = dx_s[...]
    for off in range(1, 8):
        remote(dx_s, dx_r.at[tp], dx_send, dx_recv, dp, (tp + off) % 8).start()

    def shared_in(n, carry):
        cols = pl.ds(pl.multiple_of(n * QUARTER, 128), QUARTER)
        blocks = pl.ds(n * 16, 16)
        parts = (
            mm(tok[:, cols], shw[blocks, :, 0:SHID].reshape(QUARTER, SHID)),
            mm(tok[:, cols], shw[blocks, :, SPAD : SPAD + SHID].reshape(QUARTER, SHID)),
            mm(cot[:, cols], shw[blocks, :, 2 * SPAD : 2 * SPAD + SHID].reshape(QUARTER, SHID)),
        )
        for m, part in enumerate(parts):
            sh_acc[m] = part + jnp.where(n == 0, 0.0, 1.0) * sh_acc[m]
        return carry

    for m in range(3):
        sh_acc[m] = jnp.zeros((TOK, SHID), F32)
    lax.fori_loop(0, XS, shared_in, 0)
    active, slope = silu_pair(sh_acc[0])
    sh_grad = sh_acc[2]
    sh_hid = (active * sh_acc[1]).astype(BF16)
    sh_gg = (sh_grad * sh_acc[1] * slope).astype(BF16)
    sh_gu = (sh_grad * active).astype(BF16)
    dot_high, dot_low = halves(sh_hid.astype(F32) * sh_grad)
    ones_s = jnp.ones((8, SHID), BF16)
    sx_s[...] = nt(ones_s, dot_high) + nt(ones_s, dot_low)
    sx_r[tp] = sx_s[...]
    for off in range(1, 8):
        remote(sx_s, sx_r.at[tp], sx_send, sx_recv, dp, (tp + off) % 8).start()

    rs_forward(3)
    give_back(2)

    def shared_out(q):
        blocks = pl.ds(q * 16, 16)
        out = nt(sh_hid, shw[blocks, :, 2 * SPAD : 2 * SPAD + SHID].reshape(QUARTER, SHID))
        grad = nt(sh_gg, shw[blocks, :, 0:SHID].reshape(QUARTER, SHID))
        grad = grad + nt(sh_gu, shw[blocks, :, SPAD : SPAD + SHID].reshape(QUARTER, SHID))
        return jnp.concatenate([out * scale, grad * scale], axis=1)

    def s_copy(n, src, dst, t):
        return remote(src, dst, s_send.at[n], s_recv.at[n], dp, t)

    top, low_ = slice(0, 64), slice(64, TOK)
    def own_half(v):
        low = jnp.concatenate([v[:, 0:EIGHTH], v[:, QUARTER : QUARTER + EIGHTH]], axis=1)
        high = jnp.concatenate([v[:, EIGHTH:QUARTER], v[:, QUARTER + EIGHTH :]], axis=1)
        return jnp.where(c == 0, low, high), jnp.where(c == 0, high, low)

    pair = []
    for n, q in enumerate((x2, x1, x3, x)):
        kept, given = own_half(shared_out(q))
        keep[n] = kept
        ps_s[n] = given.astype(BF16)
        pair.append(remote(ps_s.at[n], ps_r.at[n], ps_send.at[n], ps_recv.at[n], dp, x * 2 + 1 - c))
        go(pair[n])

    def pair_sum(n):
        pair[n].wait_recv()
        return keep[n] + ps_r[n].astype(F32)

    sh_s[0] = pair_sum(0).astype(BF16)
    go(s_copy(0, sh_s.at[0, top], sh_r.at[0, top], right))
    go(s_copy(1, sh_s.at[0, low_], sh_r.at[0, low_], left))
    sh_s[1] = pair_sum(1).astype(BF16)
    go(s_copy(2, sh_s.at[1, low_], sh_r.at[1, low_], right))
    sh_s[2] = pair_sum(2).astype(BF16)
    go(s_copy(3, sh_s.at[2, top], sh_r.at[2, top], left))
    shared_own = pair_sum(3)

    give_back(3)

    s_copy(0, sh_s.at[0, top], sh_r.at[0, top], left).wait_recv()
    add_part(sh_s, (1, top), sh_r[0, top])
    go(s_copy(4, sh_s.at[1, top], sh_r.at[1, top], right))
    s_copy(1, sh_s.at[0, low_], sh_r.at[0, low_], right).wait_recv()
    add_part(sh_s, (2, low_), sh_r[0, low_])
    go(s_copy(5, sh_s.at[2, low_], sh_r.at[2, low_], left))

    rank_t = rank1.T.astype(BF16)
    w_high, w_low = halves(gate_w.T)
    wide_t = nt(rank_t, spread)
    gate_t = nt(w_high, spread) + nt(w_low, spread)
    weigh_main = jnp.where(wide_t == (iota((TOK, MAIN), 1) % 8 + 1).astype(F32), gate_t, 0.0)
    spread9 = one_hot(iota((HALF, 64), 1) == c * HALF + peer_of(iota((HALF, 64), 0)))
    wide9_t = nt(rank_t, spread9)
    gate9_t = nt(w_high, spread9) + nt(w_low, spread9)
    weigh_nine = jnp.where(wide9_t == float(CAP), gate9_t, 0.0)
    main_high, main_low = halves(weigh_main)
    nine_high, nine_low = halves(weigh_nine)

    drain(dx_r.at[0:7], dx_recv)
    even = dx_r[0] + dx_r[2] + dx_r[4] + dx_r[6]
    odd = dx_r[1] + dx_r[3] + dx_r[5] + dx_r[7]
    slot_dots = jnp.concatenate([even, odd], axis=0)
    drain(sx_r.at[0:7], sx_recv)
    sh_dots = jnp.sum(sx_r[...], axis=0).T[:, 0:1]
    taken = chosen * slot_dots
    dlogits = prob * (taken - jnp.sum(gate_w * slot_dots, axis=0, keepdims=True))
    l_high, l_low = halves(dlogits.T)
    router_q = mm(slot_expert, router[:, pl.ds(pl.multiple_of(tp * EIGHTH, 128), EIGHTH)]).astype(BF16)
    grad = mm(l_high, router_q) + mm(l_low, router_q)
    sg_cols = sgate[:, pl.ds(pl.multiple_of(tp * EIGHTH, 128), EIGHTH)]
    grad = grad + sh_dots * scale * (1.0 - scale) * sg_cols

    s_copy(2, sh_s.at[1, low_], sh_r.at[1, low_], left).wait_recv()
    s_copy(3, sh_s.at[2, top], sh_r.at[2, top], right).wait_recv()
    s_copy(4, sh_s.at[1, top], sh_r.at[1, top], left).wait_recv()
    s_copy(5, sh_s.at[2, low_], sh_r.at[2, low_], right).wait_recv()
    shared_own = shared_own + sh_r[1].astype(F32) + sh_r[2].astype(F32)

    for g in range(SETS):
        drain(ret_r.at[0:8], t_recv.at[g])
    unpack_into(xrow, ret_r[...])
    total = mm(main_high, xrow[0:MAIN, :]) + mm(main_low, xrow[0:MAIN, :])
    total = total + mm(nine_high, xrow[MAIN:ROWS, :]) + mm(nine_low, xrow[MAIN:ROWS, :])
    own, px_s[...] = own_half(total)
    px = remote(px_s, px_r, px_sem.at[0], px_sem.at[1], dp, x * 2 + 1 - c)
    px.start()
    px.wait_recv()
    both = own + px_r[...] + shared_own
    result[:, :EIGHTH] = both[:, :EIGHTH].astype(BF16)
    result[:, EIGHTH:] = (both[:, EIGHTH:] + grad).astype(BF16)

    a2a_sent(send, d_send)
    a2a_sent(ret_s, t_send)
    a2a_sent(dot_s, o_send)
    for copy in (*w_copies, *sent, px):
        copy.wait_send()
    for k in range(4):
        part = shw.at[0] if k < 3 else shw.at[0, 0:16]
        drain(part, pr_send.at[k])
        drain(part, pl_send.at[k])
    for n in range(7):
        drain(shw.at[0:4], ra_send.at[n])
        drain(shw.at[0:4], la_send.at[n if n < 6 else 7])
    drain(dx_r.at[0:7], dx_send)
    drain(sx_r.at[0:7], sx_send)


def shards(
    tokens, grad_out, route_ids, expert_map, router, shared_gate, sh_gate, sh_up, sh_down, ex_gate, ex_up, ex_down
):
    vmem = pl.BlockSpec(memory_space=pltpu.VMEM)
    hbm = pl.BlockSpec(memory_space=pl.ANY)
    dma = pltpu.SemaphoreType.DMA
    block = (HALF, 8, PACK)
    sums = pl.pallas_call(
        body,
        out_shape=jax.ShapeDtypeStruct((TOK, QUARTER), BF16),
        in_specs=[vmem] * 9 + [hbm] * 3,
        out_specs=vmem,
        scratch_shapes=[
            pltpu.VMEM(block, BF16),
            pltpu.VMEM((XS, *block), BF16),
            pltpu.VMEM((2, HID, WIDTH), BF16),
            pltpu.VMEM((2, HID, WIDTH), BF16),
            pltpu.VMEM((2, HID, WIDTH), BF16),
            pltpu.VMEM((ROWS, 2 * QUARTER), BF16),
            pltpu.VMEM((6, ROWS, HID), F32),
            pltpu.VMEM((2, ROWS, HID), BF16),
            pltpu.VMEM((2, ROWS, HID), BF16),
            pltpu.VMEM((2, ROWS, HID), BF16),
            pltpu.VMEM((3, *block), BF16),
            pltpu.VMEM((SETS, 4, 8, PACK), BF16),
            pltpu.VMEM((SETS, 4, 8, PACK), BF16),
            pltpu.VMEM(block, BF16),
            pltpu.VMEM(block, BF16),
            pltpu.VMEM(block, BF16),
            pltpu.VMEM(block, BF16),
            pltpu.VMEM((RING * RING, 32, 3 * SPAD), BF16),
            pltpu.VMEM((32, 3 * SPAD), BF16),
            pltpu.VMEM((1, WIDTH), F32),
            pltpu.VMEM((3, TOK, QUARTER), BF16),
            pltpu.VMEM((3, TOK, QUARTER), BF16),
            pltpu.VMEM((4, TOK, QUARTER), F32),
            pltpu.VMEM((4, TOK, QUARTER), BF16),
            pltpu.VMEM((4, TOK, QUARTER), BF16),
            pltpu.VMEM((TOK, QUARTER), F32),
            pltpu.VMEM((TOK, QUARTER), F32),
            pltpu.VMEM((HALF, TOK), F32),
            pltpu.VMEM((8, HALF, TOK), F32),
            pltpu.VMEM((3, TOK, SHID), F32),
            pltpu.VMEM((HALF, 8, 128), BF16),
            pltpu.VMEM((HALF, 8, 128), BF16),
            pltpu.VMEM((8, TOK), F32),
            pltpu.VMEM((8, 8, TOK), F32),
            dma((4,)), dma((3,)), dma((3,)), dma, dma((4,)), dma((24,)), dma((24,)), dma((24,)), dma((24,)),
            dma, dma((4,)), dma((4,)), dma((4,)), dma((4,)), dma((4,)), dma((8,)), dma((8,)), dma((8,)), dma((8,)),
            dma((6,)), dma((6,)), dma((2,)), dma, dma, dma, dma, dma, dma, dma((4,)), dma((4,)),
        ],
        compiler_params=pltpu.CompilerParams(
            collective_id=0, has_side_effects=True, vmem_limit_bytes=60 * 1024 * 1024
        ),
    )(
        tokens, grad_out, route_ids.T, expert_map.reshape(1, 60), router.T, shared_gate.reshape(16, 128),
        sh_gate, sh_up, sh_down.T,
        ex_gate.reshape(WIDTH, HID).T, ex_up.reshape(WIDTH, HID).T, ex_down.reshape(HID, WIDTH),
    )
    return sums[:, :EIGHTH], sums[:, EIGHTH:]


def solution(mesh):
    placed = (
        P("dp", None), P("dp", None), P("dp", None), P(), P(), P(),
        P("dp", "tensor"), P("dp", "tensor"), P("tensor", "dp"),
        P("dp", None, "tensor"), P("dp", None, "tensor"), P("dp", "tensor", None),
    )
    return jax.shard_map(
        shards,
        mesh=mesh,
        in_specs=placed,
        out_specs=(P("dp", "tensor"), P("dp", "tensor")),
        check_vma=False,
    )
```
